64 devices in a mesh: dp: 4 (over x, y), cp: 16 (over z, core).
Axes of the slice: x: 2, y: 2, z: 8, core: 2. Of those that a mesh axis runs over, the one named last changes fastest.
The devices are a block of a 4x4x8 slice.
Arguments:
- hidden: bfloat16 [32768, 4096], P(('dp', 'cp')), parts along dimension 0
- grad_out: bfloat16 [32768, 4096], P(('dp', 'cp')), parts along dimension 0
- w_query: bfloat16 [4096, 4, 128], replicated
- w_key: bfloat16 [4096, 1, 128], replicated
- w_value: bfloat16 [4096, 1, 128], replicated
- w_out: bfloat16 [4, 128, 4096], replicated
Outputs:
- output 1: bfloat16 [32768, 4096], P(('dp', 'cp')), parts along dimension 0
- output 2: bfloat16 [32768, 4096], P(('dp', 'cp')), parts along dimension 0
- output 3: float32 [16384, 4, 128], P('dp'), parts along dimension 0
- output 4: float32 [16384, 1, 128], P('dp'), parts along dimension 0
- output 5: float32 [16384, 1, 128], P('dp'), parts along dimension 0
- output 6: float32 [16, 128, 4096], P('dp'), parts along dimension 0
There are 4 independent parts. The reference program is written for one: setup_inputs(seed, part) draws one part's arguments, and reference() takes and returns one part's arrays. A program takes and returns all parts, laid end to end along the dimension named above; an argument that names none is the same for every part.
All inputs are finite; a program needn't handle non-finite values.
Results may differ from the reference program's by a relative error of at most 0.010751.
Values are sent between devices in bfloat16 or wider.
A program may use at most 768 MiB of HBM per device.

```python
import jax
import jax.numpy as jnp
from jax import lax

TOKENS_DEV = 512
CP = 16
D = 4096
HEADS = 4
KV_HEADS = 1
HEAD = 128


def setup_inputs(seed: int = 0, part: int = 0) -> dict:
    seq_len = TOKENS_DEV * CP
    part_key = jax.random.fold_in(jax.random.key(seed), part)
    key_hidden, key_grad = jax.random.split(part_key)
    key_wq, key_wk, key_wv, key_wo = jax.random.split(jax.random.key(seed + 1), 4)
    hidden = jax.random.normal(key_hidden, (seq_len, D), jnp.float32)
    grad_out = jax.random.normal(key_grad, (seq_len, D), jnp.float32)
    w_query = jax.random.normal(key_wq, (D, HEADS, HEAD), jnp.float32) * D ** -0.5
    w_key = jax.random.normal(key_wk, (D, KV_HEADS, HEAD), jnp.float32) * D ** -0.5
    w_value = jax.random.normal(key_wv, (D, KV_HEADS, HEAD), jnp.float32) * D ** -0.5
    w_out = jax.random.normal(key_wo, (HEADS, HEAD, D), jnp.float32) * (HEADS * HEAD) ** -0.5
    return {
        "hidden": hidden.astype(jnp.bfloat16),
        "grad_out": grad_out.astype(jnp.bfloat16),
        "w_query": w_query.astype(jnp.bfloat16),
        "w_key": w_key.astype(jnp.bfloat16),
        "w_value": w_value.astype(jnp.bfloat16),
        "w_out": w_out.astype(jnp.bfloat16),
    }


def token_positions():
    half_len = TOKENS_DEV // 2
    row_ids = jnp.arange(TOKENS_DEV * CP)
    owner_dev = row_ids // TOKENS_DEV
    within = row_ids % TOKENS_DEV
    block_idx = jnp.where(within < half_len, owner_dev, 2 * CP - 1 - owner_dev)
    return block_idx * half_len + within % half_len


def reference(hidden, grad_out, w_query, w_key, w_value, w_out):
    seq_len = TOKENS_DEV * CP
    half_len = TOKENS_DEV // 2
    num_blocks = 2 * CP
    group_size = HEADS // KV_HEADS
    score_scale = HEAD ** -0.5
    positions = token_positions()
    wq_flat = w_query.reshape(D, HEADS * HEAD)
    wk_flat = w_key.reshape(D, KV_HEADS * HEAD)
    wv_flat = w_value.reshape(D, KV_HEADS * HEAD)
    wo_flat = w_out.reshape(HEADS * HEAD, D)
    query_all = jnp.dot(hidden, wq_flat, preferred_element_type=jnp.float32).astype(jnp.bfloat16)
    keys_all = jnp.dot(hidden, wk_flat, preferred_element_type=jnp.float32).astype(jnp.bfloat16)
    values_all = jnp.dot(hidden, wv_flat, preferred_element_type=jnp.float32).astype(jnp.bfloat16)
    keys_wide = keys_all.reshape(seq_len, KV_HEADS, HEAD).astype(jnp.float32)
    values_wide = values_all.reshape(seq_len, KV_HEADS, HEAD).astype(jnp.float32)
    query_blocks = query_all.reshape(num_blocks, half_len, KV_HEADS, group_size, HEAD)
    pos_blocks = positions.reshape(num_blocks, half_len)

    def masked_scores(query_block, pos_block):
        scores = jnp.einsum("qkgd,skd->kgqs", query_block.astype(jnp.float32), keys_wide) * score_scale
        visible = pos_block[:, None] >= positions[None, :]
        return jnp.where(visible, scores, -jnp.inf)

    def forward_block(items):
        query_block, pos_block = items
        masked = masked_scores(query_block, pos_block)
        log_norm = jax.nn.logsumexp(masked, axis=-1)
        att_probs = jnp.exp(masked - log_norm[..., None]).astype(jnp.bfloat16)
        attended = jnp.einsum("kgqs,skd->qkgd", att_probs.astype(jnp.float32), values_wide)
        return attended.astype(jnp.bfloat16), log_norm

    att_blocks, norm_blocks = lax.map(forward_block, (query_blocks, pos_blocks))
    attended = att_blocks.reshape(seq_len, HEADS * HEAD)
    output = jnp.dot(attended, wo_flat, preferred_element_type=jnp.float32).astype(jnp.bfloat16)
    d_att = jnp.dot(grad_out, wo_flat.T, preferred_element_type=jnp.float32).astype(jnp.bfloat16)
    delta_rows = jnp.sum(
        d_att.astype(jnp.float32).reshape(seq_len, KV_HEADS, group_size, HEAD)
        * attended.astype(jnp.float32).reshape(seq_len, KV_HEADS, group_size, HEAD),
        axis=-1,
    )
    delta_blocks = jnp.transpose(delta_rows.reshape(num_blocks, half_len, KV_HEADS, group_size), (0, 2, 3, 1))
    dout_blocks = d_att.reshape(num_blocks, half_len, KV_HEADS, group_size, HEAD)

    def backward_block(carry, items):
        key_acc, value_acc = carry
        query_block, pos_block, log_norm, dout_block, delta_block = items
        masked = masked_scores(query_block, pos_block)
        att_probs = jnp.exp(masked - log_norm[..., None]).astype(jnp.bfloat16).astype(jnp.float32)
        dout_wide = dout_block.astype(jnp.float32)
        d_probs = jnp.einsum("qkgd,skd->kgqs", dout_wide, values_wide)
        d_scores = (att_probs * (d_probs - delta_block[..., None])).astype(jnp.bfloat16).astype(jnp.float32)
        query_grad = (jnp.einsum("kgqs,skd->qkgd", d_scores, keys_wide) * score_scale).astype(jnp.bfloat16)
        key_acc = key_acc + jnp.einsum("kgqs,qkgd->skd", d_scores, query_block.astype(jnp.float32)) * score_scale
        value_acc = value_acc + jnp.einsum("kgqs,qkgd->skd", att_probs, dout_wide)
        return (key_acc, value_acc), query_grad

    zero_acc = jnp.zeros((seq_len, KV_HEADS, HEAD), jnp.float32)
    (key_sum, value_sum), query_grads = lax.scan(
        backward_block, (zero_acc, zero_acc), (query_blocks, pos_blocks, norm_blocks, dout_blocks, delta_blocks)
    )
    query_grad = query_grads.reshape(seq_len, HEADS * HEAD)
    key_grad = key_sum.astype(jnp.bfloat16).reshape(seq_len, KV_HEADS * HEAD)
    value_grad = value_sum.astype(jnp.bfloat16).reshape(seq_len, KV_HEADS * HEAD)
    grad_hidden = (
        jnp.dot(query_grad, wq_flat.T, preferred_element_type=jnp.float32)
        + jnp.dot(key_grad, wk_flat.T, preferred_element_type=jnp.float32)
        + jnp.dot(value_grad, wv_flat.T, preferred_element_type=jnp.float32)
    ).astype(jnp.bfloat16)
    grad_w_query = jnp.dot(hidden.T, query_grad, preferred_element_type=jnp.float32).reshape(D, HEADS, HEAD)
    grad_w_key = jnp.dot(hidden.T, key_grad, preferred_element_type=jnp.float32).reshape(D, KV_HEADS, HEAD)
    grad_w_value = jnp.dot(hidden.T, value_grad, preferred_element_type=jnp.float32).reshape(D, KV_HEADS, HEAD)
    grad_w_out = jnp.dot(attended.T, grad_out, preferred_element_type=jnp.float32).reshape(HEADS, HEAD, D)
    return (output, grad_hidden, grad_w_query, grad_w_key, grad_w_value, grad_w_out)
```

```python
import functools
import math

import jax
import jax.numpy as jnp
from jax import lax
from jax.experimental import pallas as pl
from jax.experimental.pallas import tpu as pltpu
from jax.sharding import PartitionSpec as P

F32 = jnp.float32
BF16 = jnp.bfloat16
MESH = pl.DeviceIdType.MESH
HBM = pl.BlockSpec(memory_space=pl.ANY)


def dot(a, b):
    return jnp.dot(a, b, preferred_element_type=F32)


def dot_nt(a, b):
    return lax.dot_general(a, b, (((1,), (1,)), ((), ())), preferred_element_type=F32)


def layer_kernel(
    n, heads, x_hbm, dy_hbm, wq_hbm, wk_hbm, wv_hbm, wo_hbm,
    y_hbm, dx_hbm, gq_hbm, gk_hbm, gv_hbm, go_hbm,
    x, dy, wqkv, wo, kv, q_rows, q_cols, do_rows, do_cols, o_rows, o_cols,
    acc, m_state, l_state, delta, dqkv, p_cols, ds_cols, slot_o, part_o, arena, part_w, x_cols, stage,
    in_sem, kv_send, kv_recv, ro_send, ro_recv, go_send, go_recv, rkv_send, rkv_recv,
    rw_send, rw_recv, gw_send, gw_recv, out_o_sem, out_w_sem, stage_sem, ready_sem,
):
    tok, width = x.shape
    half = tok // 2
    embed = wo.shape[0]
    hd = embed // heads
    kvw = wqkv.shape[1] - embed
    mc = width // n
    me_half = mc // 2
    cols = heads * half
    scale = hd ** -0.5
    scale2 = scale * math.log2(math.e)
    steps_right = n // 2
    steps_left = n - 1 - n // 2
    me = lax.axis_index("cp")
    right = lax.rem(me + 1, n)
    left = lax.rem(me + n - 1, n)
    target = (right, left)

    def wrap(i):
        return lax.rem(i + 2 * n, n)

    def rcopy(src, dst, send, recv, direction):
        return pltpu.make_async_remote_copy(
            src_ref=src, dst_ref=dst, send_sem=send, recv_sem=recv,
            device_id={"cp": target[direction]}, device_id_type=MESH,
        )

    def rs_chunk(direction, t):
        return wrap(me - 1 - t) if direction == 0 else wrap(me + 1 + t)

    def ag_chunk(direction, t):
        return wrap(me - t) if direction == 0 else wrap(me + t)

    loads = [
        pltpu.make_async_copy(x_hbm, x, in_sem.at[0]),
        pltpu.make_async_copy(wk_hbm, wqkv.at[:, pl.ds(embed, kvw // 2)], in_sem.at[1]),
        pltpu.make_async_copy(wv_hbm, wqkv.at[:, pl.ds(embed + kvw // 2, kvw // 2)], in_sem.at[2]),
        pltpu.make_async_copy(wq_hbm, wqkv.at[:, pl.ds(0, embed)], in_sem.at[3]),
        pltpu.make_async_copy(dy_hbm, dy, in_sem.at[4]),
        pltpu.make_async_copy(wo_hbm, wo, in_sem.at[5]),
    ]
    for load in loads:
        load.start()

    barrier = pltpu.get_barrier_semaphore()
    for device in target:
        pl.semaphore_signal(barrier, inc=1, device_id={"cp": device}, device_id_type=MESH)

    for load in loads[:3]:
        load.wait()

    kv[me] = dot(x[...], wqkv[:, embed:]).astype(BF16)
    pl.semaphore_wait(barrier, 2)

    def kv_copy(direction, t):
        c = ag_chunk(direction, t)
        return rcopy(kv.at[c], kv.at[c], kv_send.at[direction, t], kv_recv.at[direction, t], direction)

    def kv_tick(t):
        for direction, steps in ((0, steps_right), (1, steps_left)):
            @pl.when(t < steps)
            def _(direction=direction, steps=steps):
                kv_copy(direction, t).wait_recv()

                @pl.when(t + 1 < steps)
                def _():
                    kv_copy(direction, t + 1).start()

    for direction in (0, 1):
        kv_copy(direction, 0).start()

    def spread(block, rows_ref, cols_ref, h):
        for b in range(2):
            piece = block[b * half:(b + 1) * half]
            rows_ref[b, h * half:(h + 1) * half, :] = piece
            cols_ref[b, :, h * half:(h + 1) * half] = piece.T

    per = 256 // hd

    def project_q(g):
        block = dot(x[...], wqkv[:, g * 256:(g + 1) * 256]).astype(BF16)
        for i in range(per):
            spread(block[:, i * hd:(i + 1) * hd], q_rows, q_cols, g * per + i)

    def project_do(g):
        block = dot_nt(dy[...], wo[g * 256:(g + 1) * 256, :]).astype(BF16)
        for i in range(per):
            spread(block[:, i * hd:(i + 1) * hd], do_rows, do_cols, g * per + i)

    loads[3].wait()
    for g in range(embed // 256):
        project_q(g)
        if g == 0:
            kv_tick(0)
    loads[4].wait()
    loads[5].wait()
    for g in range(embed // 256):
        project_do(g)
        if g == 0:
            kv_tick(1)
    early = 2

    m_state[...] = jnp.full(m_state.shape, -jnp.inf, F32)
    l_state[...] = jnp.zeros(l_state.shape, F32)
    acc[...] = jnp.zeros(acc.shape, F32)

    def diagonal():
        key_id = lax.broadcasted_iota(jnp.int32, (half, half), 0)
        query_id = lax.broadcasted_iota(jnp.int32, (half, half), 1)
        return key_id <= query_id

    def forward_unit(s, qb, kb, masked):
        keys = kv[s, pl.ds(kb * half, half), :hd]
        values_t = kv[s, pl.ds(kb * half, half), hd:].T
        for h in range(heads):
            lanes = slice(h * half, (h + 1) * half)
            sc = dot(keys, q_cols[qb, :, lanes])
            if masked:
                sc = jnp.where(diagonal(), sc, -jnp.inf)
            old = m_state[qb, :, lanes]
            new = jnp.maximum(old, jnp.max(sc, axis=0, keepdims=True) * scale2)
            fade = jnp.exp2(old - new)
            p = jnp.exp2(sc * scale2 - new)
            l_state[qb, :, lanes] = l_state[qb, :, lanes] * fade + jnp.sum(p, axis=0, keepdims=True)
            m_state[qb, :, lanes] = new
            acc[qb, :, lanes] = acc[qb, :, lanes] * fade + dot(values_t, p.astype(BF16))

    forward_unit(me, 1, 0, False)
    forward_unit(me, 0, 0, True)
    forward_unit(me, 1, 1, True)

    def unit_blocks(s, u):
        same = jnp.where(s < me, 0, 1)
        return jnp.where(u == 0, 1, same), jnp.where(u == 0, 0, same)

    def forward_step(j, carry):
        k = j // 2

        @pl.when(lax.rem(j, 2) == 0)
        def _():
            kv_tick(k + early)

        s = jnp.where(lax.rem(j, 2) == 0, wrap(me - 1 - k), wrap(me + 1 + k))

        def unit(u, c):
            qb, kb = unit_blocks(s, u)
            forward_unit(s, qb, kb, False)
            return c

        return lax.fori_loop(0, 2, unit, carry)

    lax.fori_loop(0, n - 1, forward_step, 0)

    for direction, steps in ((0, steps_right), (1, steps_left)):
        def drain(t, c, direction=direction):
            kv_copy(direction, t).wait_send()
            return c
        lax.fori_loop(0, steps, drain, 0)

    for b in range(2):
        for h in range(heads):
            lanes = slice(h * half, (h + 1) * half)
            total = l_state[b, :, lanes]
            out = (acc[b, :, lanes] / total).astype(BF16)
            o_cols[h * hd:(h + 1) * hd, b * half:(b + 1) * half] = out
            o_rows[b * half:(b + 1) * half, h * hd:(h + 1) * hd] = out.T
            delta[b, :, lanes] = jnp.sum(
                out.astype(F32) * do_cols[b, :, lanes].astype(F32), axis=0, keepdims=True
            )
            m_state[b, :, lanes] = m_state[b, :, lanes] + jnp.log(total) * math.log2(math.e)

    eh = embed // 2

    def wo_part(t):
        for direction in (0, 1):
            c = rs_chunk(direction, t)
            at = pl.ds(pl.multiple_of(c * mc, mc), mc)
            part_o[direction] = dot(o_cols[direction * eh:(direction + 1) * eh, :], dy[:, at])

    def ro_copy(direction, t):
        c = rs_chunk(direction, t)
        return rcopy(slot_o.at[direction, c], slot_o.at[direction, c],
                     ro_send.at[direction, t], ro_recv.at[direction, t], direction)

    def wait_sends(copy, t):
        for direction in (0, 1):
            copy(direction, t).wait_send()

    def ro_tick(t):
        for direction in (0, 1):
            c = rs_chunk(direction, t)
            ro_copy(direction, t - 1).wait_recv()
            slot_o[direction, c] = slot_o[direction, c] + part_o[direction]

    wo_part(0)
    for direction in (0, 1):
        slot_o[direction, rs_chunk(direction, 0)] = part_o[direction]
        ro_copy(direction, 0).start()
    wo_part(1)

    part_kv0 = 0
    slot_kv0 = 2 * n * tok

    def kv_rows(base, direction, c):
        return pl.multiple_of(base + (direction * n + c) * tok, tok)

    acc[...] = jnp.zeros(acc.shape, F32)

    def backward_unit(s, qb, kb, masked, add):
        keys = kv[s, pl.ds(kb * half, half), :hd]
        values = kv[s, pl.ds(kb * half, half), hd:]
        keys_t = keys.T
        for h in range(heads):
            lanes = slice(h * half, (h + 1) * half)
            sc = dot(keys, q_cols[qb, :, lanes])
            p = jnp.exp2(sc * scale2 - m_state[qb, :, lanes])
            if masked:
                p = jnp.where(diagonal(), p, 0.0)
            p = p.astype(BF16)
            p_cols[:, lanes] = p
            dp = dot(values, do_cols[qb, :, lanes])
            ds = (p.astype(F32) * (dp - delta[qb, :, lanes])).astype(BF16)
            ds_cols[:, lanes] = ds
            acc[qb, :, lanes] = acc[qb, :, lanes] + dot(keys_t, ds)
        for direction, lhs, rhs in ((0, ds_cols, q_rows), (1, p_cols, do_rows)):
            rows = pl.ds(pl.multiple_of(kv_rows(part_kv0, direction, s) + kb * half, half), half)
            g = dot(lhs[...], rhs[qb])
            arena[rows, :] = arena[rows, :] + g if add else g

    def zero_block(s, kb):
        for direction in (0, 1):
            rows = pl.ds(pl.multiple_of(kv_rows(part_kv0, direction, s) + kb * half, half), half)
            arena[rows, :] = jnp.zeros((half, hd), F32)

    backward_unit(me, 1, 0, False, False)
    backward_unit(me, 0, 0, True, True)
    backward_unit(me, 1, 1, True, False)

    def backward_step(j, carry):
        s = wrap(me + j)

        @pl.when(jnp.logical_and(j >= 2, j < n - 1))
        def _():
            wait_sends(ro_copy, j - 2)

        @pl.when(j < n - 1)
        def _():
            ro_tick(j)
            for direction in (0, 1):
                ro_copy(direction, j).start()
            wo_part(j + 1)

        zero_block(s, 0)
        zero_block(s, 1)

        def unit(u, c):
            qb, kb = unit_blocks(s, u)
            backward_unit(s, qb, kb, False, True)
            return c

        return lax.fori_loop(0, 2, unit, carry)

    lax.fori_loop(1, n, backward_step, 0)

    for b in range(2):
        for h in range(heads):
            g = (acc[b, :, h * half:(h + 1) * half] * scale).astype(BF16)
            dqkv[b * half:(b + 1) * half, h * hd:(h + 1) * hd] = g.T

    def rkv_copy(direction, t):
        rows = pl.ds(kv_rows(slot_kv0, direction, rs_chunk(direction, t)), tok)
        return rcopy(arena.at[rows], arena.at[rows], rkv_send.at[direction, t], rkv_recv.at[direction, t], direction)

    def rkv_add(direction, c):
        slot = pl.ds(kv_rows(slot_kv0, direction, c), tok)
        part = pl.ds(kv_rows(part_kv0, direction, c), tok)
        return arena[slot, :] + arena[part, :]

    def go_copy(direction, t):
        c = ag_chunk(direction, t)
        return rcopy(slot_o.at[direction, c], slot_o.at[direction, c],
                     go_send.at[direction, t], go_recv.at[direction, t], direction)

    def go_out(direction, t):
        c = ag_chunk(direction, t)
        return pltpu.make_async_copy(
            slot_o.at[direction, c],
            go_hbm.at[pl.ds(direction * eh, eh), pl.ds(pl.multiple_of(c * mc, mc), mc)],
            out_o_sem.at[direction, t],
        )

    def stage_copy(dst, i):
        return pltpu.make_async_copy(
            stage.at[lax.rem(i, 2)], dst.at[:, pl.ds(pl.multiple_of(i * mc, mc), mc)], stage_sem.at[lax.rem(i, 2)]
        )

    def y_piece(i):
        stage[lax.rem(i, 2)] = dot(o_rows[...], wo[:, pl.ds(pl.multiple_of(i * mc, mc), mc)]).astype(BF16)
        stage_copy(y_hbm, i).start()

    for direction in (0, 1):
        c = rs_chunk(direction, 0)
        arena[pl.ds(kv_rows(slot_kv0, direction, c), tok), :] = arena[pl.ds(kv_rows(part_kv0, direction, c), tok), :]
        rkv_copy(direction, 0).start()
    ro_tick(n - 1)
    for direction in (0, 1):
        go_copy(direction, 0).start()
        go_out(direction, 0).start()
    y_piece(0)
    y_piece(1)

    def second_step(t, carry):
        for direction in (0, 1):
            c = rs_chunk(direction, t)
            rkv_copy(direction, t - 1).wait_recv()
            arena[pl.ds(kv_rows(slot_kv0, direction, c), tok), :] = rkv_add(direction, c)
            rkv_copy(direction, t).start()

        @pl.when(t <= 2)
        def _():
            wait_sends(ro_copy, n - 4 + t)

        for direction in (0, 1):
            go_copy(direction, t - 1).wait_recv()
            go_copy(direction, t).start()
            go_out(direction, t).start()
        stage_copy(y_hbm, t - 1).wait()
        y_piece(t + 1)
        return carry

    lax.fori_loop(1, n - 1, second_step, 0)

    for direction in (0, 1):
        rkv_copy(direction, n - 2).wait_recv()
        g = rkv_add(direction, me)
        if direction == 0:
            g = g * scale
        dqkv[:, embed + direction * hd:embed + (direction + 1) * hd] = g.astype(BF16)

    def drain_kv(t, c):
        for direction in (0, 1):
            rkv_copy(direction, t).wait_send()
        return c

    lax.fori_loop(0, n - 1, drain_kv, 0)
    for device in target:
        pl.semaphore_signal(ready_sem, inc=1, device_id={"cp": device}, device_id_type=MESH)

    wrow = me_half * (heads + 2)

    def w_rows(direction, c):
        return pl.multiple_of((direction * n + c) * wrow, wrow)

    def w_part(t):
        for direction in (0, 1):
            c = rs_chunk(direction, t)
            at = pl.ds(pl.multiple_of(c * mc + direction * me_half, me_half), me_half)
            x_cols[...] = x[:, at].T
            for g in range((embed + kvw) // 256):
                block = dot(x_cols[...], dqkv[:, g * 256:(g + 1) * 256])
                for i in range(per):
                    h = g * per + i
                    piece = block[:, i * hd:(i + 1) * hd]
                    if h < heads:
                        part_w[direction, pl.ds(h, me_half, stride=heads), :] = piece
                    else:
                        part_w[direction, pl.ds(h * me_half, me_half), :] = piece

    def rw_copy(direction, t):
        rows = pl.ds(w_rows(direction, rs_chunk(direction, t)), wrow)
        return rcopy(arena.at[rows], arena.at[rows], rw_send.at[direction, t], rw_recv.at[direction, t], direction)

    def rw_tick(t):
        for direction in (0, 1):
            rows = pl.ds(w_rows(direction, rs_chunk(direction, t)), wrow)
            rw_copy(direction, t - 1).wait_recv()
            arena[rows, :] = arena[rows, :] + part_w[direction]

    def gw_copy(direction, t):
        rows = pl.ds(w_rows(direction, ag_chunk(direction, t)), wrow)
        return rcopy(arena.at[rows], arena.at[rows], gw_send.at[direction, t], gw_recv.at[direction, t], direction)

    def gw_out(direction, t):
        c = ag_chunk(direction, t)
        row = w_rows(direction, c)
        first = c * mc + direction * me_half
        return [
            pltpu.make_async_copy(
                arena.at[pl.ds(row + skip * me_half, rows * me_half)],
                dst.at[pl.ds(pl.multiple_of(first * rows, me_half), rows * me_half)],
                out_w_sem.at[direction, t, k],
            )
            for k, (dst, skip, rows) in enumerate(((gq_hbm, 0, heads), (gk_hbm, heads, 1), (gv_hbm, heads + 1, 1)))
        ]

    w_part(0)
    pl.semaphore_wait(ready_sem, 2)
    for direction in (0, 1):
        arena[pl.ds(w_rows(direction, rs_chunk(direction, 0)), wrow), :] = part_w[direction]
        rw_copy(direction, 0).start()
    w_part(1)

    for direction in (0, 1):
        go_copy(direction, n - 2).wait_recv()
        go_out(direction, n - 1).start()
    stage_copy(y_hbm, n - 2).wait()
    stage_copy(y_hbm, n - 1).wait()

    def third_step(t, carry):
        @pl.when(t >= 2)
        def _():
            wait_sends(rw_copy, t - 2)

        rw_tick(t)
        for direction in (0, 1):
            rw_copy(direction, t).start()
        w_part(t + 1)
        return carry

    lax.fori_loop(1, n - 1, third_step, 0)

    def dx_piece(i):
        at = pl.ds(pl.multiple_of(i * mc, mc), mc)
        stage[lax.rem(i, 2)] = dot_nt(dqkv[...], wqkv[at, :]).astype(BF16)
        stage_copy(dx_hbm, i).start()

    rw_tick(n - 1)
    for direction in (0, 1):
        gw_copy(direction, 0).start()
        for copy in gw_out(direction, 0):
            copy.start()
    dx_piece(0)
    dx_piece(1)

    def fourth_step(t, carry):
        @pl.when(t <= 2)
        def _():
            wait_sends(rw_copy, n - 4 + t)

        for direction in (0, 1):
            gw_copy(direction, t - 1).wait_recv()
            gw_copy(direction, t).start()
            for copy in gw_out(direction, t):
                copy.start()
        stage_copy(dx_hbm, t - 1).wait()
        dx_piece(t + 1)
        return carry

    lax.fori_loop(1, n - 1, fourth_step, 0)

    stage_copy(dx_hbm, n - 2).wait()
    stage_copy(dx_hbm, n - 1).wait()

    def drain_all(t, c):
        for direction in (0, 1):
            go_copy(direction, t).wait_send()
            gw_copy(direction, t).wait_send()
            go_out(direction, t).wait()
        return c

    lax.fori_loop(0, n - 1, drain_all, 0)
    for direction in (0, 1):
        go_out(direction, n - 1).wait()
        gw_copy(direction, n - 2).wait_recv()
        for copy in gw_out(direction, n - 1):
            copy.start()

    def drain_out(t, c):
        for direction in (0, 1):
            for copy in gw_out(direction, t):
                copy.wait()
        return c

    lax.fori_loop(0, n, drain_out, 0)


def solution(mesh):
    n = mesh.shape["cp"]
    row_spec = P(("dp", "cp"), None)
    rep_spec = P(None, None, None)
    part_spec = P("dp", None, None)

    def device_layer(hidden, grad_out, w_query, w_key, w_value, w_out):
        tok, width = hidden.shape
        heads, hd = w_query.shape[1], w_query.shape[2]
        embed = heads * hd
        kvw = 2 * hd
        half = tok // 2
        cols = heads * half
        mc = width // n
        wrow = mc // 2 * (heads + 2)
        dma = lambda *shape: pltpu.SemaphoreType.DMA(shape)
        ring = dma(2, n - 1)
        outs = pl.pallas_call(
            functools.partial(layer_kernel, n, heads),
            name="attention_layer",
            out_shape=[
                jax.ShapeDtypeStruct((tok, width), BF16),
                jax.ShapeDtypeStruct((tok, width), BF16),
                jax.ShapeDtypeStruct((width * heads, hd), F32),
                jax.ShapeDtypeStruct((width, hd), F32),
                jax.ShapeDtypeStruct((width, hd), F32),
                jax.ShapeDtypeStruct((embed, width), F32),
            ],
            in_specs=[HBM] * 6,
            out_specs=[HBM] * 6,
            scratch_shapes=[
                pltpu.VMEM((tok, width), BF16),
                pltpu.VMEM((tok, width), BF16),
                pltpu.VMEM((width, embed + kvw), BF16),
                pltpu.VMEM((embed, width), BF16),
                pltpu.VMEM((n, tok, kvw), BF16),
                pltpu.VMEM((2, cols, hd), BF16),
                pltpu.VMEM((2, hd, cols), BF16),
                pltpu.VMEM((2, cols, hd), BF16),
                pltpu.VMEM((2, hd, cols), BF16),
                pltpu.VMEM((tok, embed), BF16),
                pltpu.VMEM((embed, tok), BF16),
                pltpu.VMEM((2, hd, cols), F32),
                pltpu.VMEM((2, 1, cols), F32),
                pltpu.VMEM((2, 1, cols), F32),
                pltpu.VMEM((2, 1, cols), F32),
                pltpu.VMEM((tok, embed + kvw), BF16),
                pltpu.VMEM((half, cols), BF16),
                pltpu.VMEM((half, cols), BF16),
                pltpu.VMEM((2, n, embed // 2, mc), F32),
                pltpu.VMEM((2, embed // 2, mc), F32),
                pltpu.VMEM((max(4 * n * tok, 2 * n * wrow), hd), F32),
                pltpu.VMEM((2, wrow, hd), F32),
                pltpu.VMEM((mc // 2, tok), BF16),
                pltpu.VMEM((2, tok, mc), BF16),
                dma(6),
                dma(2, n // 2), dma(2, n // 2),
                ring, ring, ring, ring, ring, ring, ring, ring, ring, ring,
                dma(2, n), dma(2, n, 3), dma(2),
                pltpu.SemaphoreType.REGULAR,
            ],
            compiler_params=pltpu.CompilerParams(
                collective_id=0, has_side_effects=True, vmem_limit_bytes=67_000_000
            ),
        )(
            hidden, grad_out, w_query.reshape(width, embed), w_key.reshape(width, hd), w_value.reshape(width, hd),
            w_out.reshape(embed, width),
        )
        output, grad_hidden, gq, gk, gv, go = outs
        return (
            output,
            grad_hidden,
            gq.reshape(width, heads, hd),
            gk.reshape(width, 1, hd),
            gv.reshape(width, 1, hd),
            go.reshape(heads, hd, width),
        )

    return jax.shard_map(
        device_layer,
        mesh=mesh,
        in_specs=(row_spec, row_spec, rep_spec, rep_spec, rep_spec, rep_spec),
        out_specs=(row_spec, row_spec, part_spec, part_spec, part_spec, part_spec),
        check_vma=False,
    )
```

```python
import functools
import math

import jax
import jax.numpy as jnp
from jax import lax
from jax.experimental import pallas as pl
from jax.experimental.pallas import tpu as pltpu
from jax.sharding import PartitionSpec as P

F32 = jnp.float32
BF16 = jnp.bfloat16
MESH = pl.DeviceIdType.MESH
HBM = pl.BlockSpec(memory_space=pl.ANY)


def dot(a, b):
    return jnp.dot(a, b, preferred_element_type=F32)


def dot_nt(a, b):
    return lax.dot_general(a, b, (((1,), (1,)), ((), ())), preferred_element_type=F32)


def layer_kernel(
    n, heads, x_hbm, dy_hbm, wq_hbm, wk_hbm, wv_hbm, wo_hbm,
    y_hbm, dx_hbm, gq_hbm, gk_hbm, gv_hbm, go_hbm,
    x, dy, wqkv, wo, kv, q_rows, q_cols, do_rows, do_cols, o_rows, o_cols,
    acc, m_state, l_state, delta, dqkv, p_cols, ds_cols, slot_o, part_o, arena, part_w, x_cols, stage,
    in_sem, kv_send, kv_recv, ro_send, ro_recv, go_send, go_recv, rkv_send, rkv_recv,
    rw_send, rw_recv, gw_send, gw_recv, out_o_sem, out_w_sem, stage_sem, ready_sem,
):
    tok, width = x.shape
    half = tok // 2
    embed = wo.shape[0]
    hd = embed // heads
    kvw = wqkv.shape[1] - embed
    mc = width // n
    me_half = mc // 2
    cols = heads * half
    scale = hd ** -0.5
    scale2 = scale * math.log2(math.e)
    me = lax.axis_index("cp")
    right = lax.rem(me + 1, n)
    left = lax.rem(me + n - 1, n)
    second = lax.rem(me, 2)
    first = 1 - second
    order = (first, second)

    def wrap(i):
        return lax.rem(i + 2 * n, n)

    def rcopy(src, dst, send, recv, direction):
        return pltpu.make_async_remote_copy(
            src_ref=src, dst_ref=dst, send_sem=send, recv_sem=recv,
            device_id={"cp": right + direction * (left - right)}, device_id_type=MESH,
        )

    def rs_chunk(direction, t):
        return wrap(me + (2 * direction - 1) * (t + 1))

    def ag_chunk(direction, t):
        return wrap(me + (2 * direction - 1) * t)

    loads = [
        pltpu.make_async_copy(x_hbm, x, in_sem.at[0]),
        pltpu.make_async_copy(wk_hbm, wqkv.at[:, pl.ds(embed, kvw // 2)], in_sem.at[1]),
        pltpu.make_async_copy(wv_hbm, wqkv.at[:, pl.ds(embed + kvw // 2, kvw // 2)], in_sem.at[2]),
        pltpu.make_async_copy(wq_hbm, wqkv.at[:, pl.ds(0, embed)], in_sem.at[3]),
        pltpu.make_async_copy(dy_hbm, dy, in_sem.at[4]),
        pltpu.make_async_copy(wo_hbm, wo, in_sem.at[5]),
    ]
    for load in loads:
        load.start()

    barrier = pltpu.get_barrier_semaphore()
    for device in (left, right):
        pl.semaphore_signal(barrier, inc=1, device_id={"cp": device}, device_id_type=MESH)

    for load in loads[:3]:
        load.wait()

    kv[me] = dot(x[...], wqkv[:, embed:]).astype(BF16)
    pl.semaphore_wait(barrier, 2)

    def kv_copy(direction, t):
        c = ag_chunk(direction, t)
        return rcopy(kv.at[c], kv.at[c], kv_send.at[direction, t], kv_recv.at[direction, t], direction)

    def kv_steps(direction):
        return n // 2 + direction * (n - 1 - 2 * (n // 2))

    def kv_tick(direction, t):
        @pl.when(t < kv_steps(direction))
        def _():
            kv_copy(direction, t).wait_recv()

            @pl.when(t + 1 < kv_steps(direction))
            def _():
                kv_copy(direction, t + 1).start()

    for direction in order:
        kv_copy(direction, 0).start()

    def spread(block, rows_ref, cols_ref, h):
        for b in range(2):
            piece = block[b * half:(b + 1) * half]
            rows_ref[b, h * half:(h + 1) * half, :] = piece
            cols_ref[b, :, h * half:(h + 1) * half] = piece.T

    per = 256 // hd

    def project_q(g):
        block = dot(x[...], wqkv[:, g * 256:(g + 1) * 256]).astype(BF16)
        for i in range(per):
            spread(block[:, i * hd:(i + 1) * hd], q_rows, q_cols, g * per + i)

    def project_do(g):
        block = dot_nt(dy[...], wo[g * 256:(g + 1) * 256, :]).astype(BF16)
        for i in range(per):
            spread(block[:, i * hd:(i + 1) * hd], do_rows, do_cols, g * per + i)

    loads[3].wait()
    for g in range(embed // 256):
        project_q(g)
        kv_tick(order[g % 2], g // 2)
    loads[4].wait()
    loads[5].wait()
    for g in range(embed // 256):
        project_do(g)
        kv_tick(order[g % 2], embed // 512 + g // 2)
    early = embed // 256

    m_state[...] = jnp.full(m_state.shape, -jnp.inf, F32)
    l_state[...] = jnp.zeros(l_state.shape, F32)
    acc[...] = jnp.zeros(acc.shape, F32)

    def diagonal():
        key_id = lax.broadcasted_iota(jnp.int32, (half, half), 0)
        query_id = lax.broadcasted_iota(jnp.int32, (half, half), 1)
        return key_id <= query_id

    def forward_unit(s, qb, kb, masked):
        keys = kv[s, pl.ds(kb * half, half), :hd]
        values_t = kv[s, pl.ds(kb * half, half), hd:].T
        for h in range(heads):
            lanes = slice(h * half, (h + 1) * half)
            sc = dot(keys, q_cols[qb, :, lanes])
            if masked:
                sc = jnp.where(diagonal(), sc, -jnp.inf)
            old = m_state[qb, :, lanes]
            new = jnp.maximum(old, jnp.max(sc, axis=0, keepdims=True) * scale2)
            fade = jnp.exp2(old - new)
            p = jnp.exp2(sc * scale2 - new)
            l_state[qb, :, lanes] = l_state[qb, :, lanes] * fade + jnp.sum(p, axis=0, keepdims=True)
            m_state[qb, :, lanes] = new
            acc[qb, :, lanes] = acc[qb, :, lanes] * fade + dot(values_t, p.astype(BF16))

    forward_unit(me, 1, 0, False)
    forward_unit(me, 0, 0, True)
    forward_unit(me, 1, 1, True)

    def unit_blocks(s, u):
        same = jnp.where(s < me, 0, 1)
        return jnp.where(u == 0, 1, same), jnp.where(u == 0, 0, same)

    def forward_step(j, carry):
        direction = first + lax.rem(j, 2) * (second - first)
        kv_tick(direction, j // 2 + early)
        s = rs_chunk(direction, j // 2)

        def unit(u, c):
            qb, kb = unit_blocks(s, u)
            forward_unit(s, qb, kb, False)
            return c

        return lax.fori_loop(0, 2, unit, carry)

    lax.fori_loop(0, n - 1, forward_step, 0)

    for direction in (0, 1):
        def drain(t, c, direction=direction):
            kv_copy(direction, t).wait_send()
            return c

        lax.fori_loop(0, kv_steps(direction), drain, 0)

    for b in range(2):
        for h in range(heads):
            lanes = slice(h * half, (h + 1) * half)
            total = l_state[b, :, lanes]
            out = (acc[b, :, lanes] / total).astype(BF16)
            o_cols[h * hd:(h + 1) * hd, b * half:(b + 1) * half] = out
            o_rows[b * half:(b + 1) * half, h * hd:(h + 1) * hd] = out.T
            delta[b, :, lanes] = jnp.sum(
                out.astype(F32) * do_cols[b, :, lanes].astype(F32), axis=0, keepdims=True
            )
            m_state[b, :, lanes] = m_state[b, :, lanes] + jnp.log(total) * math.log2(math.e)

    eh = embed // 2

    def wo_part(direction, t):
        at = pl.ds(pl.multiple_of(rs_chunk(direction, t) * mc, mc), mc)
        rows = pl.ds(pl.multiple_of(direction * eh, eh), eh)
        part_o[direction] = dot(o_cols[rows, :], dy[:, at])

    def ro_copy(direction, t):
        c = rs_chunk(direction, t)
        return rcopy(slot_o.at[direction, c], slot_o.at[direction, c],
                     ro_send.at[direction, t], ro_recv.at[direction, t], direction)

    def wait_sends(copy, t):
        for direction in (0, 1):
            copy(direction, t).wait_send()

    def ro_tick(direction, t):
        c = rs_chunk(direction, t)
        ro_copy(direction, t - 1).wait_recv()
        slot_o[direction, c] = slot_o[direction, c] + part_o[direction]

    for direction in order:
        wo_part(direction, 0)
        slot_o[direction, rs_chunk(direction, 0)] = part_o[direction]
        ro_copy(direction, 0).start()
    for direction in order:
        wo_part(direction, 1)

    part_kv0 = 0
    slot_kv0 = 2 * n * tok

    def kv_rows(base, direction, c):
        return pl.multiple_of(base + (direction * n + c) * tok, tok)

    acc[...] = jnp.zeros(acc.shape, F32)

    def backward_unit(s, qb, kb, masked, add):
        keys = kv[s, pl.ds(kb * half, half), :hd]
        values = kv[s, pl.ds(kb * half, half), hd:]
        keys_t = keys.T
        for h in range(heads):
            lanes = slice(h * half, (h + 1) * half)
            sc = dot(keys, q_cols[qb, :, lanes])
            p = jnp.exp2(sc * scale2 - m_state[qb, :, lanes])
            if masked:
                p = jnp.where(diagonal(), p, 0.0)
            p = p.astype(BF16)
            p_cols[:, lanes] = p
            dp = dot(values, do_cols[qb, :, lanes])
            ds = (p.astype(F32) * (dp - delta[qb, :, lanes])).astype(BF16)
            ds_cols[:, lanes] = ds
            acc[qb, :, lanes] = acc[qb, :, lanes] + dot(keys_t, ds)
        for direction, lhs, rhs in ((0, ds_cols, q_rows), (1, p_cols, do_rows)):
            rows = pl.ds(pl.multiple_of(kv_rows(part_kv0, direction, s) + kb * half, half), half)
            g = dot(lhs[...], rhs[qb])
            arena[rows, :] = arena[rows, :] + g if add else g

    def zero_block(s, kb):
        for direction in (0, 1):
            rows = pl.ds(pl.multiple_of(kv_rows(part_kv0, direction, s) + kb * half, half), half)
            arena[rows, :] = jnp.zeros((half, hd), F32)

    backward_unit(me, 1, 0, False, False)
    backward_unit(me, 0, 0, True, True)
    backward_unit(me, 1, 1, True, False)

    def backward_step(j, carry):
        s = wrap(me + j)

        @pl.when(jnp.logical_and(j >= 2, j < n - 1))
        def _():
            wait_sends(ro_copy, j - 2)

        zero_block(s, 0)
        zero_block(s, 1)

        def unit(u, c):
            direction = first + u * (second - first)

            @pl.when(j < n - 1)
            def _():
                ro_tick(direction, j)
                ro_copy(direction, j).start()
                wo_part(direction, j + 1)

            qb, kb = unit_blocks(s, u)
            backward_unit(s, qb, kb, False, True)
            return c

        return lax.fori_loop(0, 2, unit, carry)

    lax.fori_loop(1, n, backward_step, 0)

    for b in range(2):
        for h in range(heads):
            g = (acc[b, :, h * half:(h + 1) * half] * scale).astype(BF16)
            dqkv[b * half:(b + 1) * half, h * hd:(h + 1) * hd] = g.T

    def rkv_copy(direction, t):
        rows = pl.ds(kv_rows(slot_kv0, direction, rs_chunk(direction, t)), tok)
        return rcopy(arena.at[rows], arena.at[rows], rkv_send.at[direction, t], rkv_recv.at[direction, t], direction)

    def rkv_add(direction, c):
        slot = pl.ds(kv_rows(slot_kv0, direction, c), tok)
        part = pl.ds(kv_rows(part_kv0, direction, c), tok)
        return arena[slot, :] + arena[part, :]

    def go_copy(direction, t):
        c = ag_chunk(direction, t)
        return rcopy(slot_o.at[direction, c], slot_o.at[direction, c],
                     go_send.at[direction, t], go_recv.at[direction, t], direction)

    def go_out(direction, t):
        c = ag_chunk(direction, t)
        return pltpu.make_async_copy(
            slot_o.at[direction, c],
            go_hbm.at[pl.ds(direction * eh, eh), pl.ds(pl.multiple_of(c * mc, mc), mc)],
            out_o_sem.at[direction, t],
        )

    def stage_copy(dst, i):
        return pltpu.make_async_copy(
            stage.at[lax.rem(i, 2)], dst.at[:, pl.ds(pl.multiple_of(i * mc, mc), mc)], stage_sem.at[lax.rem(i, 2)]
        )

    def y_piece(i):
        stage[lax.rem(i, 2)] = dot(o_rows[...], wo[:, pl.ds(pl.multiple_of(i * mc, mc), mc)]).astype(BF16)
        stage_copy(y_hbm, i).start()

    for direction in order:
        c = rs_chunk(direction, 0)
        arena[pl.ds(kv_rows(slot_kv0, direction, c), tok), :] = arena[pl.ds(kv_rows(part_kv0, direction, c), tok), :]
        rkv_copy(direction, 0).start()
    for direction in order:
        ro_tick(direction, n - 1)
        go_copy(direction, 0).start()
        go_out(direction, 0).start()
    y_piece(0)
    y_piece(1)

    def second_step(t, carry):
        for direction in order:
            c = rs_chunk(direction, t)
            rkv_copy(direction, t - 1).wait_recv()
            arena[pl.ds(kv_rows(slot_kv0, direction, c), tok), :] = rkv_add(direction, c)
            rkv_copy(direction, t).start()

        @pl.when(t <= 2)
        def _():
            wait_sends(ro_copy, n - 4 + t)

        for direction in order:
            go_copy(direction, t - 1).wait_recv()
            go_copy(direction, t).start()
            go_out(direction, t).start()
        stage_copy(y_hbm, t - 1).wait()
        y_piece(t + 1)
        return carry

    lax.fori_loop(1, n - 1, second_step, 0)

    for direction in (0, 1):
        rkv_copy(direction, n - 2).wait_recv()
        g = rkv_add(direction, me)
        if direction == 0:
            g = g * scale
        dqkv[:, embed + direction * hd:embed + (direction + 1) * hd] = g.astype(BF16)

    def drain_kv(t, c):
        for direction in (0, 1):
            rkv_copy(direction, t).wait_send()
        return c

    lax.fori_loop(0, n - 1, drain_kv, 0)
    for device in (left, right):
        pl.semaphore_signal(ready_sem, inc=1, device_id={"cp": device}, device_id_type=MESH)

    wrow = me_half * (heads + 2)

    def w_rows(direction, c):
        return pl.multiple_of((direction * n + c) * wrow, wrow)

    def w_part(direction, t):
        c = rs_chunk(direction, t)
        at = pl.ds(pl.multiple_of(c * mc + direction * me_half, me_half), me_half)
        x_cols[...] = x[:, at].T
        for g in range((embed + kvw) // 256):
            block = dot(x_cols[...], dqkv[:, g * 256:(g + 1) * 256])
            for i in range(per):
                h = g * per + i
                piece = block[:, i * hd:(i + 1) * hd]
                if h < heads:
                    part_w[direction, pl.ds(h, me_half, stride=heads), :] = piece
                else:
                    part_w[direction, pl.ds(h * me_half, me_half), :] = piece

    def rw_copy(direction, t):
        rows = pl.ds(w_rows(direction, rs_chunk(direction, t)), wrow)
        return rcopy(arena.at[rows], arena.at[rows], rw_send.at[direction, t], rw_recv.at[direction, t], direction)

    def rw_tick(direction, t):
        rows = pl.ds(w_rows(direction, rs_chunk(direction, t)), wrow)
        rw_copy(direction, t - 1).wait_recv()
        arena[rows, :] = arena[rows, :] + part_w[direction]

    def gw_copy(direction, t):
        rows = pl.ds(w_rows(direction, ag_chunk(direction, t)), wrow)
        return rcopy(arena.at[rows], arena.at[rows], gw_send.at[direction, t], gw_recv.at[direction, t], direction)

    def gw_out(direction, t):
        c = ag_chunk(direction, t)
        row = w_rows(direction, c)
        first = c * mc + direction * me_half
        return [
            pltpu.make_async_copy(
                arena.at[pl.ds(row + skip * me_half, rows * me_half)],
                dst.at[pl.ds(pl.multiple_of(first * rows, me_half), rows * me_half)],
                out_w_sem.at[direction, t, k],
            )
            for k, (dst, skip, rows) in enumerate(((gq_hbm, 0, heads), (gk_hbm, heads, 1), (gv_hbm, heads + 1, 1)))
        ]

    w_part(first, 0)
    pl.semaphore_wait(ready_sem, 2)
    for direction in order:
        if direction is second:
            w_part(second, 0)
        arena[pl.ds(w_rows(direction, rs_chunk(direction, 0)), wrow), :] = part_w[direction]
        rw_copy(direction, 0).start()
    for direction in order:
        w_part(direction, 1)

    for direction in (0, 1):
        go_copy(direction, n - 2).wait_recv()
        go_out(direction, n - 1).start()
    stage_copy(y_hbm, n - 2).wait()
    stage_copy(y_hbm, n - 1).wait()

    def third_step(t, carry):
        @pl.when(t >= 2)
        def _():
            wait_sends(rw_copy, t - 2)

        for direction in order:
            rw_tick(direction, t)
            rw_copy(direction, t).start()
            w_part(direction, t + 1)
        return carry

    lax.fori_loop(1, n - 1, third_step, 0)

    def dx_piece(i):
        at = pl.ds(pl.multiple_of(i * mc, mc), mc)
        stage[lax.rem(i, 2)] = dot_nt(dqkv[...], wqkv[at, :]).astype(BF16)
        stage_copy(dx_hbm, i).start()

    for direction in order:
        rw_tick(direction, n - 1)
        gw_copy(direction, 0).start()
        for copy in gw_out(direction, 0):
            copy.start()
    dx_piece(0)
    dx_piece(1)

    def fourth_step(t, carry):
        @pl.when(t <= 2)
        def _():
            wait_sends(rw_copy, n - 4 + t)

        for direction in order:
            gw_copy(direction, t - 1).wait_recv()
            gw_copy(direction, t).start()
            for copy in gw_out(direction, t):
                copy.start()
        stage_copy(dx_hbm, t - 1).wait()
        dx_piece(t + 1)
        return carry

    lax.fori_loop(1, n - 1, fourth_step, 0)

    stage_copy(dx_hbm, n - 2).wait()
    stage_copy(dx_hbm, n - 1).wait()

    def drain_all(t, c):
        for direction in (0, 1):
            go_copy(direction, t).wait_send()
            gw_copy(direction, t).wait_send()
            go_out(direction, t).wait()
        return c

    lax.fori_loop(0, n - 1, drain_all, 0)
    for direction in (0, 1):
        go_out(direction, n - 1).wait()
        gw_copy(direction, n - 2).wait_recv()
        for copy in gw_out(direction, n - 1):
            copy.start()

    def drain_out(t, c):
        for direction in (0, 1):
            for copy in gw_out(direction, t):
                copy.wait()
        return c

    lax.fori_loop(0, n, drain_out, 0)


def solution(mesh):
    n = mesh.shape["cp"]
    row_spec = P(("dp", "cp"), None)
    rep_spec = P(None, None, None)
    part_spec = P("dp", None, None)

    def device_layer(hidden, grad_out, w_query, w_key, w_value, w_out):
        tok, width = hidden.shape
        heads, hd = w_query.shape[1], w_query.shape[2]
        embed = heads * hd
        kvw = 2 * hd
        half = tok // 2
        cols = heads * half
        mc = width // n
        wrow = mc // 2 * (heads + 2)
        dma = lambda *shape: pltpu.SemaphoreType.DMA(shape)
        ring = dma(2, n - 1)
        outs = pl.pallas_call(
            functools.partial(layer_kernel, n, heads),
            name="attention_layer",
            out_shape=[
                jax.ShapeDtypeStruct((tok, width), BF16),
                jax.ShapeDtypeStruct((tok, width), BF16),
                jax.ShapeDtypeStruct((width * heads, hd), F32),
                jax.ShapeDtypeStruct((width, hd), F32),
                jax.ShapeDtypeStruct((width, hd), F32),
                jax.ShapeDtypeStruct((embed, width), F32),
            ],
            in_specs=[HBM] * 6,
            out_specs=[HBM] * 6,
            scratch_shapes=[
                pltpu.VMEM((tok, width), BF16),
                pltpu.VMEM((tok, width), BF16),
                pltpu.VMEM((width, embed + kvw), BF16),
                pltpu.VMEM((embed, width), BF16),
                pltpu.VMEM((n, tok, kvw), BF16),
                pltpu.VMEM((2, cols, hd), BF16),
                pltpu.VMEM((2, hd, cols), BF16),
                pltpu.VMEM((2, cols, hd), BF16),
                pltpu.VMEM((2, hd, cols), BF16),
                pltpu.VMEM((tok, embed), BF16),
                pltpu.VMEM((embed, tok), BF16),
                pltpu.VMEM((2, hd, cols), F32),
                pltpu.VMEM((2, 1, cols), F32),
                pltpu.VMEM((2, 1, cols), F32),
                pltpu.VMEM((2, 1, cols), F32),
                pltpu.VMEM((tok, embed + kvw), BF16),
                pltpu.VMEM((half, cols), BF16),
                pltpu.VMEM((half, cols), BF16),
                pltpu.VMEM((2, n, embed // 2, mc), F32),
                pltpu.VMEM((2, embed // 2, mc), F32),
                pltpu.VMEM((max(4 * n * tok, 2 * n * wrow), hd), F32),
                pltpu.VMEM((2, wrow, hd), F32),
                pltpu.VMEM((mc // 2, tok), BF16),
                pltpu.VMEM((2, tok, mc), BF16),
                dma(6),
                dma(2, n // 2), dma(2, n // 2),
                ring, ring, ring, ring, ring, ring, ring, ring, ring, ring,
                dma(2, n), dma(2, n, 3), dma(2),
                pltpu.SemaphoreType.REGULAR,
            ],
            compiler_params=pltpu.CompilerParams(
                collective_id=0, has_side_effects=True, vmem_limit_bytes=67_000_000
            ),
        )(
            hidden, grad_out, w_query.reshape(width, embed), w_key.reshape(width, hd), w_value.reshape(width, hd),
            w_out.reshape(embed, width),
        )
        output, grad_hidden, gq, gk, gv, go = outs
        return (
            output,
            grad_hidden,
            gq.reshape(width, heads, hd),
            gk.reshape(width, 1, hd),
            gv.reshape(width, 1, hd),
            go.reshape(heads, hd, width),
        )

    return jax.shard_map(
        device_layer,
        mesh=mesh,
        in_specs=(row_spec, row_spec, rep_spec, rep_spec, rep_spec, rep_spec),
        out_specs=(row_spec, row_spec, part_spec, part_spec, part_spec, part_spec),
        check_vma=False,
    )
```

```python
import functools
import math

import jax
import jax.numpy as jnp
from jax import lax
from jax.experimental import pallas as pl
from jax.experimental.pallas import tpu as pltpu
from jax.sharding import PartitionSpec as P

F32 = jnp.float32
BF16 = jnp.bfloat16
MESH = pl.DeviceIdType.MESH
HBM = pl.BlockSpec(memory_space=pl.ANY)


def dot(a, b):
    return jnp.dot(a, b, preferred_element_type=F32)


def dot_nt(a, b):
    return lax.dot_general(a, b, (((1,), (1,)), ((), ())), preferred_element_type=F32)


def layer_kernel(
    n, heads, x_hbm, dy_hbm, wq_hbm, wk_hbm, wv_hbm, wo_hbm,
    y_hbm, dx_hbm, gq_hbm, gk_hbm, gv_hbm, go_hbm,
    x, dy, wqkv, wo, kv, q_rows, q_cols, do_rows, do_cols, o_rows, o_cols,
    acc, m_state, l_state, delta, dqkv, slot_o, part_o, arena, part_w, x_cols, stage, extra_ob, gift_ob, extra_kvb, extra_wb, gift_wb,
    in_sem, kv_send, kv_recv, ro_send, ro_recv, go_send, go_recv, rkv_send, rkv_recv,
    rw_send, rw_recv, gw_send, gw_recv, extra_send, extra_recv, out_o_sem, out_w_sem, stage_sem, ready_sem,
):
    tok, width = x.shape
    half = tok // 2
    embed = wo.shape[0]
    hd = embed // heads
    kvw = wqkv.shape[1] - embed
    mc = width // n
    me_half = mc // 2
    cols = heads * half
    scale = hd ** -0.5
    scale2 = scale * math.log2(math.e)
    me = lax.axis_index("cp")
    right = lax.rem(me + 1, n)
    left = lax.rem(me + n - 1, n)
    second = lax.rem(me, 2)
    first = 1 - second
    order = (first, second)

    def wrap(i):
        return lax.rem(i + 2 * n, n)

    def rcopy(src, dst, send, recv, direction):
        return pltpu.make_async_remote_copy(
            src_ref=src, dst_ref=dst, send_sem=send, recv_sem=recv,
            device_id={"cp": right + direction * (left - right)}, device_id_type=MESH,
        )

    def rs_chunk(direction, t):
        return wrap(me + (2 * direction - 1) * (t + 1))

    def ag_chunk(direction, t):
        return wrap(me + (2 * direction - 1) * t)

    loads = [
        pltpu.make_async_copy(x_hbm, x, in_sem.at[0]),
        pltpu.make_async_copy(wk_hbm, wqkv.at[:, pl.ds(embed, kvw // 2)], in_sem.at[1]),
        pltpu.make_async_copy(wv_hbm, wqkv.at[:, pl.ds(embed + kvw // 2, kvw // 2)], in_sem.at[2]),
        pltpu.make_async_copy(wq_hbm, wqkv.at[:, pl.ds(0, embed)], in_sem.at[3]),
        pltpu.make_async_copy(dy_hbm, dy, in_sem.at[4]),
        pltpu.make_async_copy(wo_hbm, wo, in_sem.at[5]),
    ]
    for load in loads[:3]:
        load.start()

    barrier = pltpu.get_barrier_semaphore()
    for device in (left, right):
        pl.semaphore_signal(barrier, inc=1, device_id={"cp": device}, device_id_type=MESH)

    for load in loads[:3]:
        load.wait()
    for load in loads[3:]:
        load.start()

    kv[me] = dot(x[...], wqkv[:, embed:]).astype(BF16)
    pl.semaphore_wait(barrier, 2)

    def kv_copy(direction, t):
        c = ag_chunk(direction, t)
        return rcopy(kv.at[c], kv.at[c], kv_send.at[direction, t], kv_recv.at[direction, t], direction)

    def kv_steps(direction):
        return n // 2 + direction * (n - 1 - 2 * (n // 2))

    def kv_tick(direction, t):
        @pl.when(t < kv_steps(direction))
        def _():
            kv_copy(direction, t).wait_recv()

            @pl.when(t + 1 < kv_steps(direction))
            def _():
                kv_copy(direction, t + 1).start()

    for direction in order:
        kv_copy(direction, 0).start()

    def spread(block, rows_ref, cols_ref, h):
        for b in range(2):
            piece = block[b * half:(b + 1) * half]
            rows_ref[b, h * half:(h + 1) * half, :] = piece
            cols_ref[b, :, h * half:(h + 1) * half] = piece.T

    per = 256 // hd

    def project_q(g):
        block = dot(x[...], wqkv[:, g * 256:(g + 1) * 256]).astype(BF16)
        for i in range(per):
            spread(block[:, i * hd:(i + 1) * hd], q_rows, q_cols, g * per + i)

    def project_do(g):
        block = dot_nt(dy[...], wo[g * 256:(g + 1) * 256, :]).astype(BF16)
        for i in range(per):
            spread(block[:, i * hd:(i + 1) * hd], do_rows, do_cols, g * per + i)

    loads[3].wait()
    for g in range(embed // 256):
        project_q(g)
        kv_tick(order[g % 2], g // 2)
    early = embed // 512

    m_state[...] = jnp.full(m_state.shape, -jnp.inf, F32)
    l_state[...] = jnp.zeros(l_state.shape, F32)
    acc[...] = jnp.zeros(acc.shape, F32)

    def diagonal():
        key_id = lax.broadcasted_iota(jnp.int32, (half, cols), 0)
        query_id = lax.rem(lax.broadcasted_iota(jnp.int32, (half, cols), 1), half)
        return key_id <= query_id

    def forward_unit(s, qb, kb, masked):
        keys = kv[s, pl.ds(kb * half, half), :hd]
        values_t = kv[s, pl.ds(kb * half, half), hd:].T
        sc = dot(keys, q_cols[qb])
        if masked:
            sc = jnp.where(diagonal(), sc, -jnp.inf)
        old = m_state[qb]
        new = jnp.maximum(old, jnp.max(sc, axis=0, keepdims=True) * scale2)
        fade = jnp.exp2(old - new)
        p = jnp.exp2(sc * scale2 - new)
        l_state[qb] = l_state[qb] * fade + jnp.sum(p, axis=0, keepdims=True)
        m_state[qb] = new
        acc[qb] = acc[qb] * fade + dot(values_t, p.astype(BF16))

    forward_unit(me, 1, 0, False)
    forward_unit(me, 0, 0, True)
    forward_unit(me, 1, 1, True)

    def unit_blocks(s, u):
        same = jnp.where(s < me, 0, 1)
        return jnp.where(u == 0, 1, same), jnp.where(u == 0, 0, same)

    def forward_step(j, carry):
        direction = first + lax.rem(j, 2) * (second - first)
        kv_tick(direction, j // 2 + early)
        s = rs_chunk(direction, j // 2)

        def unit(u, c):
            qb, kb = unit_blocks(s, u)
            forward_unit(s, qb, kb, False)
            return c

        return lax.fori_loop(0, 2, unit, carry)

    lax.fori_loop(0, n - 1, forward_step, 0)

    for direction in (0, 1):
        def drain(t, c, direction=direction):
            kv_copy(direction, t).wait_send()
            return c

        lax.fori_loop(0, kv_steps(direction), drain, 0)

    for b in range(2):
        for h in range(heads):
            lanes = slice(h * half, (h + 1) * half)
            total = l_state[b, :, lanes]
            out = (acc[b, :, lanes] / total).astype(BF16)
            o_cols[h * hd:(h + 1) * hd, b * half:(b + 1) * half] = out
            o_rows[b * half:(b + 1) * half, h * hd:(h + 1) * hd] = out.T
            m_state[b, :, lanes] = m_state[b, :, lanes] + jnp.log(total) * math.log2(math.e)

    eh = embed // 2

    def wo_part(direction, t):
        at = pl.ds(pl.multiple_of(rs_chunk(direction, t) * mc, mc), mc)
        rows = pl.ds(pl.multiple_of(direction * eh, eh), eh)
        part_o[direction] = dot(o_cols[rows, :], dy[:, at])

    def ro_copy(direction, t):
        c = rs_chunk(direction, t)
        return rcopy(slot_o.at[direction, c], slot_o.at[direction, c],
                     ro_send.at[direction, t], ro_recv.at[direction, t], direction)

    def wait_sends(copy, t):
        copy(second, t).wait_send()

        @pl.when(t > 0)
        def _():
            copy(first, t).wait_send()

    def ro_tick(direction, t):
        c = rs_chunk(direction, t)
        ro_copy(direction, t - 1).wait_recv()
        slot_o[direction, c] = slot_o[direction, c] + part_o[direction]

    def extra_copy(src, dst, k):
        return rcopy(src, dst, extra_send.at[k], extra_recv.at[k], second)

    def extra_o():
        return extra_copy(slot_o.at[first, rs_chunk(first, 0)], extra_ob, 0)

    def gift_o():
        return extra_copy(slot_o.at[first, me], gift_ob, 1)

    loads[4].wait()
    wo_part(first, 0)
    slot_o[first, rs_chunk(first, 0)] = part_o[first]
    extra_o().start()
    wo_part(second, 0)
    slot_o[second, rs_chunk(second, 0)] = part_o[second]
    ro_copy(second, 0).start()
    wo_part(second, 1)
    slot_o[second, rs_chunk(second, 1)] = part_o[second]
    wo_part(first, 1)
    ro_tick(first, 1)
    ro_copy(first, 1).start()
    ro_copy(second, 1).start()
    for direction in order:
        wo_part(direction, 2)

    loads[5].wait()
    for g in range(embed // 256):
        project_do(g)
        if g == 0:
            ro_tick(first, 2)
            ro_copy(first, 2).start()
            wo_part(first, 3)
        if g == 1:
            ro_tick(second, 2)
            ro_copy(second, 2).start()
            wo_part(second, 3)
    for b in range(2):
        for h in range(heads):
            lanes = slice(h * half, (h + 1) * half)
            out = o_cols[h * hd:(h + 1) * hd, b * half:(b + 1) * half].astype(F32)
            delta[b, :, lanes] = jnp.sum(out * do_cols[b, :, lanes].astype(F32), axis=0, keepdims=True)

    part_kv0 = 0
    slot_kv0 = 2 * n * tok

    def kv_rows(base, direction, c):
        return pl.multiple_of(base + (direction * n + c) * tok, tok)

    acc[...] = jnp.zeros(acc.shape, F32)

    def backward_unit(s, qb, kb, masked, add):
        keys = kv[s, pl.ds(kb * half, half), :hd]
        values = kv[s, pl.ds(kb * half, half), hd:]
        sc = dot(keys, q_cols[qb])
        p = jnp.exp2(sc * scale2 - m_state[qb])
        if masked:
            p = jnp.where(diagonal(), p, 0.0)
        p = p.astype(BF16)
        dp = dot(values, do_cols[qb])
        ds = (p.astype(F32) * (dp - delta[qb])).astype(BF16)
        acc[qb] = acc[qb] + dot(keys.T, ds)
        for direction, lhs, rhs in ((0, ds, q_rows), (1, p, do_rows)):
            rows = pl.ds(pl.multiple_of(kv_rows(part_kv0, direction, s) + kb * half, half), half)
            g = dot(lhs, rhs[qb])
            arena[rows, :] = arena[rows, :] + g if add else g

    def zero_block(s, kb):
        for direction in (0, 1):
            rows = pl.ds(pl.multiple_of(kv_rows(part_kv0, direction, s) + kb * half, half), half)
            arena[rows, :] = jnp.zeros((half, hd), F32)

    wait_sends(ro_copy, 0)
    extra_o().wait_send()
    backward_unit(me, 1, 0, False, False)
    backward_unit(me, 0, 0, True, True)
    backward_unit(me, 1, 1, True, False)

    def backward_step(j, carry):
        s = wrap(me + j)

        t = j + 2

        @pl.when(t < n - 1)
        def _():
            wait_sends(ro_copy, t - 2)

        zero_block(s, 0)
        zero_block(s, 1)

        def unit(u, c):
            direction = first + u * (second - first)

            @pl.when(t < n - 1)
            def _():
                ro_tick(direction, t)
                ro_copy(direction, t).start()
                wo_part(direction, t + 1)

            qb, kb = unit_blocks(s, u)
            backward_unit(s, qb, kb, False, True)
            return c

        return lax.fori_loop(0, 2, unit, carry)

    lax.fori_loop(1, n, backward_step, 0)

    for b in range(2):
        for h in range(heads):
            g = (acc[b, :, h * half:(h + 1) * half] * scale).astype(BF16)
            dqkv[b * half:(b + 1) * half, h * hd:(h + 1) * hd] = g.T

    def rkv_copy(direction, t):
        rows = pl.ds(kv_rows(slot_kv0, direction, rs_chunk(direction, t)), tok)
        return rcopy(arena.at[rows], arena.at[rows], rkv_send.at[direction, t], rkv_recv.at[direction, t], direction)

    def rkv_add(direction, c):
        slot = pl.ds(kv_rows(slot_kv0, direction, c), tok)
        part = pl.ds(kv_rows(part_kv0, direction, c), tok)
        return arena[slot, :] + arena[part, :]

    def go_copy(direction, t):
        c = ag_chunk(direction, t)
        return rcopy(slot_o.at[direction, c], slot_o.at[direction, c],
                     go_send.at[direction, t], go_recv.at[direction, t], direction)

    def go_out(direction, t):
        c = ag_chunk(direction, t)
        return pltpu.make_async_copy(
            slot_o.at[direction, c],
            go_hbm.at[pl.ds(direction * eh, eh), pl.ds(pl.multiple_of(c * mc, mc), mc)],
            out_o_sem.at[direction, t],
        )

    def stage_copy(dst, i):
        return pltpu.make_async_copy(
            stage.at[lax.rem(i, 2)], dst.at[:, pl.ds(pl.multiple_of(i * mc, mc), mc)], stage_sem.at[lax.rem(i, 2)]
        )

    def y_piece(i):
        stage[lax.rem(i, 2)] = dot(o_rows[...], wo[:, pl.ds(pl.multiple_of(i * mc, mc), mc)]).astype(BF16)
        stage_copy(y_hbm, i).start()

    def extra_kv():
        return extra_copy(arena.at[pl.ds(kv_rows(part_kv0, first, rs_chunk(first, 0)), tok)], extra_kvb, 2)

    extra_kv().start()
    for t in (0, 1):
        c = rs_chunk(second, t)
        arena[pl.ds(kv_rows(slot_kv0, second, c), tok), :] = arena[pl.ds(kv_rows(part_kv0, second, c), tok), :]
        rkv_copy(second, t).start()
    c = rs_chunk(first, 1)
    rkv_copy(first, 0).wait_recv()
    arena[pl.ds(kv_rows(slot_kv0, first, c), tok), :] = rkv_add(first, c)
    rkv_copy(first, 1).start()
    ro_tick(first, n - 1)
    go_copy(first, 0).start()
    gift_o().start()
    extra_o().wait_recv()
    part_o[second] = part_o[second] + extra_ob[...]
    ro_tick(second, n - 1)
    go_copy(second, 0).start()
    for direction in order:
        go_out(direction, 0).start()
    y_piece(0)
    y_piece(1)

    def ag_send(copy, direction, t):
        @pl.when(jnp.logical_or(t < n - 2, direction == second))
        def _():
            copy(direction, t).start()

    def second_step(t, carry):
        u = t + 1
        for direction in order:
            @pl.when(u < n - 1)
            def _(direction=direction):
                c = rs_chunk(direction, u)
                rkv_copy(direction, u - 1).wait_recv()
                arena[pl.ds(kv_rows(slot_kv0, direction, c), tok), :] = rkv_add(direction, c)
                rkv_copy(direction, u).start()

        @pl.when(t <= 2)
        def _():
            wait_sends(ro_copy, n - 4 + t)

        for direction in order:
            go_copy(direction, t - 1).wait_recv()
            ag_send(go_copy, direction, t)
            go_out(direction, t).start()
        stage_copy(y_hbm, t - 1).wait()
        y_piece(t + 1)
        return carry

    lax.fori_loop(1, n - 1, second_step, 0)

    extra_kv().wait_recv()
    mine = pl.ds(kv_rows(slot_kv0, second, me), tok)
    rkv_copy(second, n - 2).wait_recv()
    arena[mine, :] = arena[mine, :] + extra_kvb[...]
    rkv_copy(first, n - 2).wait_recv()
    for direction in (0, 1):
        g = rkv_add(direction, me)
        if direction == 0:
            g = g * scale
        dqkv[:, embed + direction * hd:embed + (direction + 1) * hd] = g.astype(BF16)

    def drain_kv(t, c):
        wait_sends(rkv_copy, t)
        return c

    lax.fori_loop(0, n - 1, drain_kv, 0)
    extra_kv().wait_send()
    for device in (left, right):
        pl.semaphore_signal(ready_sem, inc=1, device_id={"cp": device}, device_id_type=MESH)

    wrow = me_half * (heads + 2)

    def w_rows(direction, c):
        return pl.multiple_of((direction * n + c) * wrow, wrow)

    def w_part(direction, t):
        c = rs_chunk(direction, t)
        at = pl.ds(pl.multiple_of(c * mc + direction * me_half, me_half), me_half)
        x_cols[...] = x[:, at].T
        for g in range((embed + kvw) // 256):
            block = dot(x_cols[...], dqkv[:, g * 256:(g + 1) * 256])
            for i in range(per):
                h = g * per + i
                piece = block[:, i * hd:(i + 1) * hd]
                if h < heads:
                    part_w[direction, pl.ds(h, me_half, stride=heads), :] = piece
                else:
                    part_w[direction, pl.ds(h * me_half, me_half), :] = piece

    def rw_copy(direction, t):
        rows = pl.ds(w_rows(direction, rs_chunk(direction, t)), wrow)
        return rcopy(arena.at[rows], arena.at[rows], rw_send.at[direction, t], rw_recv.at[direction, t], direction)

    def rw_tick(direction, t):
        rows = pl.ds(w_rows(direction, rs_chunk(direction, t)), wrow)
        rw_copy(direction, t - 1).wait_recv()
        arena[rows, :] = arena[rows, :] + part_w[direction]

    def gw_copy(direction, t):
        rows = pl.ds(w_rows(direction, ag_chunk(direction, t)), wrow)
        return rcopy(arena.at[rows], arena.at[rows], gw_send.at[direction, t], gw_recv.at[direction, t], direction)

    def gw_out(direction, t, src=arena):
        c = ag_chunk(direction, t)
        row = w_rows(direction, c) if src is arena else 0
        start = c * mc + direction * me_half
        return [
            pltpu.make_async_copy(
                src.at[pl.ds(row + skip * me_half, rows * me_half)],
                dst.at[pl.ds(pl.multiple_of(start * rows, me_half), rows * me_half)],
                out_w_sem.at[direction, t, k],
            )
            for k, (dst, skip, rows) in enumerate(((gq_hbm, 0, heads), (gk_hbm, heads, 1), (gv_hbm, heads + 1, 1)))
        ]

    def extra_w():
        return extra_copy(arena.at[pl.ds(w_rows(first, rs_chunk(first, 0)), wrow)], extra_wb, 3)

    def gift_w():
        return extra_copy(arena.at[pl.ds(w_rows(first, me), wrow)], gift_wb, 4)

    w_part(second, 0)
    pl.semaphore_wait(ready_sem, 2)
    arena[pl.ds(w_rows(second, rs_chunk(second, 0)), wrow), :] = part_w[second]
    rw_copy(second, 0).start()
    w_part(first, 1)
    rw_tick(first, 1)
    rw_copy(first, 1).start()
    w_part(first, 0)
    arena[pl.ds(w_rows(first, rs_chunk(first, 0)), wrow), :] = part_w[first]
    extra_w().start()
    w_part(second, 1)
    arena[pl.ds(w_rows(second, rs_chunk(second, 1)), wrow), :] = part_w[second]
    rw_copy(second, 1).start()
    for direction in order:
        w_part(direction, 2)

    def last_o():
        at = pl.ds(pl.multiple_of(ag_chunk(second, n - 1) * mc, mc), mc)
        rows = pl.ds(pl.multiple_of(second * eh, eh), eh)
        return pltpu.make_async_copy(gift_ob, go_hbm.at[rows, at], out_o_sem.at[second, n - 1])

    go_copy(first, n - 2).wait_recv()
    go_out(first, n - 1).start()
    gift_o().wait_recv()
    last_o().start()
    stage_copy(y_hbm, n - 2).wait()
    stage_copy(y_hbm, n - 1).wait()

    def third_step(t, carry):
        wait_sends(rw_copy, t - 2)
        for direction in order:
            rw_tick(direction, t)
            rw_copy(direction, t).start()
            w_part(direction, t + 1)
        return carry

    extra_w().wait_send()
    lax.fori_loop(2, n - 1, third_step, 0)

    def dx_piece(i):
        at = pl.ds(pl.multiple_of(i * mc, mc), mc)
        stage[lax.rem(i, 2)] = dot_nt(dqkv[...], wqkv[at, :]).astype(BF16)
        stage_copy(dx_hbm, i).start()

    rw_tick(first, n - 1)
    gw_copy(first, 0).start()
    gift_w().start()
    extra_w().wait_recv()
    part_w[second] = part_w[second] + extra_wb[...]
    rw_tick(second, n - 1)
    gw_copy(second, 0).start()
    for direction in order:
        for copy in gw_out(direction, 0):
            copy.start()
    dx_piece(0)
    dx_piece(1)

    def fourth_step(t, carry):
        @pl.when(t <= 2)
        def _():
            wait_sends(rw_copy, n - 4 + t)

        for direction in order:
            gw_copy(direction, t - 1).wait_recv()
            ag_send(gw_copy, direction, t)
            for copy in gw_out(direction, t):
                copy.start()
        stage_copy(dx_hbm, t - 1).wait()
        dx_piece(t + 1)
        return carry

    lax.fori_loop(1, n - 1, fourth_step, 0)

    stage_copy(dx_hbm, n - 2).wait()
    stage_copy(dx_hbm, n - 1).wait()

    gw_copy(first, n - 2).wait_recv()
    gift_w().wait_recv()
    for copy in gw_out(first, n - 1) + gw_out(second, n - 1, gift_wb):
        copy.start()

    def drain_all(t, c):
        for copy in (go_copy, gw_copy):
            copy(second, t).wait_send()

            @pl.when(t < n - 2)
            def _(copy=copy):
                copy(first, t).wait_send()

        for direction in (0, 1):
            go_out(direction, t).wait()
            for copy in gw_out(direction, t):
                copy.wait()
        return c

    lax.fori_loop(0, n - 1, drain_all, 0)
    for copy in [go_out(first, n - 1), last_o()] + gw_out(first, n - 1) + gw_out(second, n - 1, gift_wb):
        copy.wait()
    for copy in (gift_o, gift_w):
        copy().wait_send()


def solution(mesh):
    n = mesh.shape["cp"]
    row_spec = P(("dp", "cp"), None)
    rep_spec = P(None, None, None)
    part_spec = P("dp", None, None)

    def device_layer(hidden, grad_out, w_query, w_key, w_value, w_out):
        tok, width = hidden.shape
        heads, hd = w_query.shape[1], w_query.shape[2]
        embed = heads * hd
        kvw = 2 * hd
        half = tok // 2
        cols = heads * half
        mc = width // n
        wrow = mc // 2 * (heads + 2)
        dma = lambda *shape: pltpu.SemaphoreType.DMA(shape)
        ring = dma(2, n - 1)
        outs = pl.pallas_call(
            functools.partial(layer_kernel, n, heads),
            name="attention_layer",
            out_shape=[
                jax.ShapeDtypeStruct((tok, width), BF16),
                jax.ShapeDtypeStruct((tok, width), BF16),
                jax.ShapeDtypeStruct((width * heads, hd), F32),
                jax.ShapeDtypeStruct((width, hd), F32),
                jax.ShapeDtypeStruct((width, hd), F32),
                jax.ShapeDtypeStruct((embed, width), F32),
            ],
            in_specs=[HBM] * 6,
            out_specs=[HBM] * 6,
            scratch_shapes=[
                pltpu.VMEM((tok, width), BF16),
                pltpu.VMEM((tok, width), BF16),
                pltpu.VMEM((width, embed + kvw), BF16),
                pltpu.VMEM((embed, width), BF16),
                pltpu.VMEM((n, tok, kvw), BF16),
                pltpu.VMEM((2, cols, hd), BF16),
                pltpu.VMEM((2, hd, cols), BF16),
                pltpu.VMEM((2, cols, hd), BF16),
                pltpu.VMEM((2, hd, cols), BF16),
                pltpu.VMEM((tok, embed), BF16),
                pltpu.VMEM((embed, tok), BF16),
                pltpu.VMEM((2, hd, cols), F32),
                pltpu.VMEM((2, 1, cols), F32),
                pltpu.VMEM((2, 1, cols), F32),
                pltpu.VMEM((2, 1, cols), F32),
                pltpu.VMEM((tok, embed + kvw), BF16),
                pltpu.VMEM((2, n, embed // 2, mc), F32),
                pltpu.VMEM((2, embed // 2, mc), F32),
                pltpu.VMEM((max(4 * n * tok, 2 * n * wrow), hd), F32),
                pltpu.VMEM((2, wrow, hd), F32),
                pltpu.VMEM((mc // 2, tok), BF16),
                pltpu.VMEM((2, tok, mc), BF16),
                pltpu.VMEM((embed // 2, mc), F32),
                pltpu.VMEM((embed // 2, mc), F32),
                pltpu.VMEM((tok, hd), F32),
                pltpu.VMEM((wrow, hd), F32),
                pltpu.VMEM((wrow, hd), F32),
                dma(6),
                dma(2, n // 2), dma(2, n // 2),
                ring, ring, ring, ring, ring, ring, ring, ring, ring, ring,
                dma(5), dma(5), dma(2, n), dma(2, n, 3), dma(2),
                pltpu.SemaphoreType.REGULAR,
            ],
            compiler_params=pltpu.CompilerParams(
                collective_id=0, has_side_effects=True, vmem_limit_bytes=67_000_000
            ),
        )(
            hidden, grad_out, w_query.reshape(width, embed), w_key.reshape(width, hd), w_value.reshape(width, hd),
            w_out.reshape(embed, width),
        )
        output, grad_hidden, gq, gk, gv, go = outs
        return (
            output,
            grad_hidden,
            gq.reshape(width, heads, hd),
            gk.reshape(width, 1, hd),
            gv.reshape(width, 1, hd),
            go.reshape(heads, hd, width),
        )

    return jax.shard_map(
        device_layer,
        mesh=mesh,
        in_specs=(row_spec, row_spec, rep_spec, rep_spec, rep_spec, rep_spec),
        out_specs=(row_spec, row_spec, part_spec, part_spec, part_spec, part_spec),
        check_vma=False,
    )
```

```python
import functools
import math

import jax
import jax.numpy as jnp
from jax import lax
from jax.experimental import pallas as pl
from jax.experimental.pallas import tpu as pltpu
from jax.sharding import PartitionSpec as P

F32 = jnp.float32
BF16 = jnp.bfloat16
MESH = pl.DeviceIdType.MESH
HBM = pl.BlockSpec(memory_space=pl.ANY)
VMEM = pl.BlockSpec(memory_space=pltpu.VMEM)


def dot(a, b):
    return jnp.dot(a, b, preferred_element_type=F32)


def dot_nt(a, b):
    return lax.dot_general(a, b, (((1,), (1,)), ((), ())), preferred_element_type=F32)


def layer_kernel(
    n, heads, x_hbm, dy_hbm, wq_hbm, wk_hbm, wv_hbm, wo_hbm,
    x, dy, slot_o, arena,
    wqkv, wo, kv, q_rows, q_cols, do_rows, do_cols, o_rows, o_cols,
    acc, m_state, l_state, delta, dqkv, part_o, part_w, x_cols, extra_ob, gift_ob, extra_kvb, extra_wb, gift_wb,
    in_sem, kv_send, kv_recv, ro_send, ro_recv, go_send, go_recv, rkv_send, rkv_recv,
    rw_send, rw_recv, gw_send, gw_recv, extra_send, extra_recv, ready_sem,
):
    tok, width = x.shape
    half = tok // 2
    embed = wo.shape[0]
    hd = embed // heads
    kvw = wqkv.shape[1] - embed
    mc = width // n
    me_half = mc // 2
    cols = heads * half
    scale = hd ** -0.5
    scale2 = scale * math.log2(math.e)
    me = lax.axis_index("cp")
    right = lax.rem(me + 1, n)
    left = lax.rem(me + n - 1, n)
    second = lax.rem(me, 2)
    first = 1 - second
    order = (first, second)

    def wrap(i):
        return lax.rem(i + 2 * n, n)

    def rcopy(src, dst, send, recv, direction):
        return pltpu.make_async_remote_copy(
            src_ref=src, dst_ref=dst, send_sem=send, recv_sem=recv,
            device_id={"cp": right + direction * (left - right)}, device_id_type=MESH,
        )

    def rs_chunk(direction, t):
        return wrap(me + (2 * direction - 1) * (t + 1))

    def ag_chunk(direction, t):
        return wrap(me + (2 * direction - 1) * t)

    loads = [
        pltpu.make_async_copy(x_hbm, x, in_sem.at[0]),
        pltpu.make_async_copy(wk_hbm, wqkv.at[:, pl.ds(embed, kvw // 2)], in_sem.at[1]),
        pltpu.make_async_copy(wv_hbm, wqkv.at[:, pl.ds(embed + kvw // 2, kvw // 2)], in_sem.at[2]),
        pltpu.make_async_copy(wq_hbm, wqkv.at[:, pl.ds(0, embed)], in_sem.at[3]),
        pltpu.make_async_copy(dy_hbm, dy, in_sem.at[4]),
        pltpu.make_async_copy(wo_hbm, wo, in_sem.at[5]),
    ]
    for load in loads[:3]:
        load.start()

    barrier = pltpu.get_barrier_semaphore()
    for device in (left, right):
        pl.semaphore_signal(barrier, inc=1, device_id={"cp": device}, device_id_type=MESH)

    for load in loads[:3]:
        load.wait()
    for load in loads[3:]:
        load.start()

    kv[me] = dot(x[...], wqkv[:, embed:]).astype(BF16)
    pl.semaphore_wait(barrier, 2)

    def kv_copy(direction, t):
        c = ag_chunk(direction, t)
        return rcopy(kv.at[c], kv.at[c], kv_send.at[direction, t], kv_recv.at[direction, t], direction)

    def kv_steps(direction):
        return n // 2 + direction * (n - 1 - 2 * (n // 2))

    def kv_tick(direction, t):
        @pl.when(t < kv_steps(direction))
        def _():
            kv_copy(direction, t).wait_recv()

            @pl.when(t + 1 < kv_steps(direction))
            def _():
                kv_copy(direction, t + 1).start()

    for direction in order:
        kv_copy(direction, 0).start()

    def spread(block, rows_ref, cols_ref, h):
        for b in range(2):
            piece = block[b * half:(b + 1) * half]
            rows_ref[b, h * half:(h + 1) * half, :] = piece
            cols_ref[b, :, h * half:(h + 1) * half] = piece.T

    per = 256 // hd

    def project_q(g):
        block = dot(x[...], wqkv[:, g * 256:(g + 1) * 256]).astype(BF16)
        for i in range(per):
            spread(block[:, i * hd:(i + 1) * hd], q_rows, q_cols, g * per + i)

    def project_do(g):
        block = dot_nt(dy[...], wo[g * 256:(g + 1) * 256, :]).astype(BF16)
        for i in range(per):
            spread(block[:, i * hd:(i + 1) * hd], do_rows, do_cols, g * per + i)

    loads[3].wait()
    for g in range(embed // 256):
        project_q(g)
        kv_tick(order[g % 2], g // 2)
    early = embed // 512

    m_state[...] = jnp.full(m_state.shape, -jnp.inf, F32)
    l_state[...] = jnp.zeros(l_state.shape, F32)
    acc[...] = jnp.zeros(acc.shape, F32)

    def diagonal():
        key_id = lax.broadcasted_iota(jnp.int32, (half, cols), 0)
        query_id = lax.rem(lax.broadcasted_iota(jnp.int32, (half, cols), 1), half)
        return key_id <= query_id

    def forward_unit(s, qb, kb, masked):
        keys = kv[s, pl.ds(kb * half, half), :hd]
        values_t = kv[s, pl.ds(kb * half, half), hd:].T
        sc = dot(keys, q_cols[qb])
        if masked:
            sc = jnp.where(diagonal(), sc, -jnp.inf)
        old = m_state[qb]
        new = jnp.maximum(old, jnp.max(sc, axis=0, keepdims=True) * scale2)
        fade = jnp.exp2(old - new)
        p = jnp.exp2(sc * scale2 - new)
        l_state[qb] = l_state[qb] * fade + jnp.sum(p, axis=0, keepdims=True)
        m_state[qb] = new
        acc[qb] = acc[qb] * fade + dot(values_t, p.astype(BF16))

    forward_unit(me, 1, 0, False)
    forward_unit(me, 0, 0, True)
    forward_unit(me, 1, 1, True)

    def unit_blocks(s, u):
        same = jnp.where(s < me, 0, 1)
        return jnp.where(u == 0, 1, same), jnp.where(u == 0, 0, same)

    def forward_step(j, carry):
        direction = first + lax.rem(j, 2) * (second - first)
        kv_tick(direction, j // 2 + early)
        s = rs_chunk(direction, j // 2)

        def unit(u, c):
            qb, kb = unit_blocks(s, u)
            forward_unit(s, qb, kb, False)
            return c

        return lax.fori_loop(0, 2, unit, carry)

    lax.fori_loop(0, n - 1, forward_step, 0)

    for direction in (0, 1):
        def drain(t, c, direction=direction):
            kv_copy(direction, t).wait_send()
            return c

        lax.fori_loop(0, kv_steps(direction), drain, 0)

    for b in range(2):
        for h in range(heads):
            lanes = slice(h * half, (h + 1) * half)
            total = l_state[b, :, lanes]
            out = (acc[b, :, lanes] / total).astype(BF16)
            o_cols[h * hd:(h + 1) * hd, b * half:(b + 1) * half] = out
            o_rows[b * half:(b + 1) * half, h * hd:(h + 1) * hd] = out.T
            m_state[b, :, lanes] = m_state[b, :, lanes] + jnp.log(total) * math.log2(math.e)

    eh = embed // 2

    es = eh // 2

    def sub_rows(sub, size):
        return pl.ds(pl.multiple_of(sub * size, size), size)

    def wo_part(direction, t, sub):
        at = pl.ds(pl.multiple_of(rs_chunk(direction, t) * mc, mc), mc)
        rows = pl.ds(pl.multiple_of(direction * eh + sub * es, es), es)
        part_o[direction, sub_rows(sub, es), :] = dot(o_cols[rows, :], dy[:, at])

    def ro_copy(direction, t, sub):
        piece = slot_o.at[direction, rs_chunk(direction, t), sub_rows(sub, es)]
        return rcopy(piece, piece, ro_send.at[direction, t, sub], ro_recv.at[direction, t, sub], direction)

    def wait_sends(copy, t):
        for sub in (0, 1):
            copy(second, t, sub).wait_send()

            @pl.when(t > 0)
            def _(sub=sub):
                copy(first, t, sub).wait_send()

    def ro_tick(direction, t, sub):
        c = rs_chunk(direction, t)
        rows = sub_rows(sub, es)
        ro_copy(direction, t - 1, sub).wait_recv()
        slot_o[direction, c, rows, :] = slot_o[direction, c, rows, :] + part_o[direction, rows, :]

    def ro_step(t, sub):
        for direction in order:
            ro_tick(direction, t, sub)
            ro_copy(direction, t, sub).start()
        for direction in order:
            wo_part(direction, t + 1, sub)

    def extra_copy(src, dst, k):
        return rcopy(src, dst, extra_send.at[k], extra_recv.at[k], second)

    def extra_o():
        return extra_copy(slot_o.at[first, rs_chunk(first, 0)], extra_ob, 0)

    def gift_o():
        return extra_copy(slot_o.at[first, me], gift_ob, 1)

    loads[4].wait()
    for sub in (0, 1):
        wo_part(second, 0, sub)
        slot_o[second, rs_chunk(second, 0), sub_rows(sub, es), :] = part_o[second, sub_rows(sub, es), :]
        ro_copy(second, 0, sub).start()
    for sub in (0, 1):
        wo_part(first, 1, sub)
        ro_tick(first, 1, sub)
        ro_copy(first, 1, sub).start()
    for sub in (0, 1):
        wo_part(second, 1, sub)
        slot_o[second, rs_chunk(second, 1), sub_rows(sub, es), :] = part_o[second, sub_rows(sub, es), :]
        ro_copy(second, 1, sub).start()
    for sub in (0, 1):
        wo_part(first, 0, sub)
    slot_o[first, rs_chunk(first, 0)] = part_o[first]
    extra_o().start()
    for sub in (0, 1):
        for direction in order:
            wo_part(direction, 2, sub)

    loads[5].wait()
    for g in range(embed // 256):
        project_do(g)
        if g < 2:
            ro_step(2, g)
    for b in range(2):
        for h in range(heads):
            lanes = slice(h * half, (h + 1) * half)
            out = o_cols[h * hd:(h + 1) * hd, b * half:(b + 1) * half].astype(F32)
            delta[b, :, lanes] = jnp.sum(out * do_cols[b, :, lanes].astype(F32), axis=0, keepdims=True)

    part_kv0 = 0
    slot_kv0 = 2 * n * tok

    def kv_rows(base, direction, c):
        return pl.multiple_of(base + (direction * n + c) * tok, tok)

    acc[...] = jnp.zeros(acc.shape, F32)

    def backward_unit(s, qb, kb, masked, add):
        keys = kv[s, pl.ds(kb * half, half), :hd]
        values = kv[s, pl.ds(kb * half, half), hd:]
        sc = dot(keys, q_cols[qb])
        p = jnp.exp2(sc * scale2 - m_state[qb])
        if masked:
            p = jnp.where(diagonal(), p, 0.0)
        p = p.astype(BF16)
        dp = dot(values, do_cols[qb])
        ds = (p.astype(F32) * (dp - delta[qb])).astype(BF16)
        acc[qb] = acc[qb] + dot(keys.T, ds)
        for direction, lhs, rhs in ((0, ds, q_rows), (1, p, do_rows)):
            rows = pl.ds(pl.multiple_of(kv_rows(part_kv0, direction, s) + kb * half, half), half)
            g = dot(lhs, rhs[qb])
            arena[rows, :] = arena[rows, :] + g if add else g

    def zero_block(s, kb):
        for direction in (0, 1):
            rows = pl.ds(pl.multiple_of(kv_rows(part_kv0, direction, s) + kb * half, half), half)
            arena[rows, :] = jnp.zeros((half, hd), F32)

    wait_sends(ro_copy, 0)
    extra_o().wait_send()
    backward_unit(me, 1, 0, False, False)
    backward_unit(me, 0, 0, True, True)
    backward_unit(me, 1, 1, True, False)

    def backward_step(j, carry):
        s = wrap(me + j)

        t = j + 2

        @pl.when(t < n - 1)
        def _():
            wait_sends(ro_copy, t - 2)

        zero_block(s, 0)
        zero_block(s, 1)

        def unit(u, c):
            @pl.when(t < n - 1)
            def _():
                ro_step(t, u)

            qb, kb = unit_blocks(s, u)
            backward_unit(s, qb, kb, False, True)
            return c

        return lax.fori_loop(0, 2, unit, carry)

    lax.fori_loop(1, n, backward_step, 0)

    for b in range(2):
        for h in range(heads):
            g = (acc[b, :, h * half:(h + 1) * half] * scale).astype(BF16)
            dqkv[b * half:(b + 1) * half, h * hd:(h + 1) * hd] = g.T

    def rkv_copy(direction, t):
        rows = pl.ds(kv_rows(slot_kv0, direction, rs_chunk(direction, t)), tok)
        return rcopy(arena.at[rows], arena.at[rows], rkv_send.at[direction, t], rkv_recv.at[direction, t], direction)

    def rkv_add(direction, c):
        slot = pl.ds(kv_rows(slot_kv0, direction, c), tok)
        part = pl.ds(kv_rows(part_kv0, direction, c), tok)
        return arena[slot, :] + arena[part, :]

    def go_copy(direction, t):
        c = ag_chunk(direction, t)
        return rcopy(slot_o.at[direction, c], slot_o.at[direction, c],
                     go_send.at[direction, t], go_recv.at[direction, t], direction)

    def y_piece(i):
        at = pl.ds(pl.multiple_of(i * mc, mc), mc)
        dy[:, at] = dot(o_rows[...], wo[:, at]).astype(BF16)

    def extra_kv():
        return extra_copy(arena.at[pl.ds(kv_rows(part_kv0, first, rs_chunk(first, 0)), tok)], extra_kvb, 2)

    extra_kv().start()
    for t in (0, 1):
        c = rs_chunk(second, t)
        arena[pl.ds(kv_rows(slot_kv0, second, c), tok), :] = arena[pl.ds(kv_rows(part_kv0, second, c), tok), :]
        rkv_copy(second, t).start()
    c = rs_chunk(first, 1)
    rkv_copy(first, 0).wait_recv()
    arena[pl.ds(kv_rows(slot_kv0, first, c), tok), :] = rkv_add(first, c)
    rkv_copy(first, 1).start()
    for sub in (0, 1):
        ro_tick(first, n - 1, sub)
    go_copy(first, 0).start()
    gift_o().start()
    extra_o().wait_recv()
    part_o[second] = part_o[second] + extra_ob[...]
    for sub in (0, 1):
        ro_tick(second, n - 1, sub)
    go_copy(second, 0).start()
    y_piece(0)
    y_piece(1)

    def ag_send(copy, direction, t):
        @pl.when(jnp.logical_or(t < n - 2, direction == second))
        def _():
            copy.start()

    def second_step(t, carry):
        u = t + 1
        for direction in order:
            @pl.when(u < n - 1)
            def _(direction=direction):
                c = rs_chunk(direction, u)
                rkv_copy(direction, u - 1).wait_recv()
                arena[pl.ds(kv_rows(slot_kv0, direction, c), tok), :] = rkv_add(direction, c)
                rkv_copy(direction, u).start()

        @pl.when(t <= 2)
        def _():
            wait_sends(ro_copy, n - 4 + t)

        for direction in order:
            go_copy(direction, t - 1).wait_recv()
            ag_send(go_copy(direction, t), direction, t)
        y_piece(t + 1)
        return carry

    lax.fori_loop(1, n - 1, second_step, 0)

    extra_kv().wait_recv()
    mine = pl.ds(kv_rows(slot_kv0, second, me), tok)
    rkv_copy(second, n - 2).wait_recv()
    arena[mine, :] = arena[mine, :] + extra_kvb[...]
    rkv_copy(first, n - 2).wait_recv()
    for direction in (0, 1):
        g = rkv_add(direction, me)
        if direction == 0:
            g = g * scale
        dqkv[:, embed + direction * hd:embed + (direction + 1) * hd] = g.astype(BF16)

    def drain_kv(t, c):
        rkv_copy(second, t).wait_send()

        @pl.when(t > 0)
        def _():
            rkv_copy(first, t).wait_send()

        return c

    lax.fori_loop(0, n - 1, drain_kv, 0)
    extra_kv().wait_send()
    for device in (left, right):
        pl.semaphore_signal(ready_sem, inc=1, device_id={"cp": device}, device_id_type=MESH)

    wrow = me_half * (heads + 2)

    def w_rows(direction, c):
        return pl.multiple_of((direction * n + c) * wrow, wrow)

    def w_part(direction, t):
        c = rs_chunk(direction, t)
        at = pl.ds(pl.multiple_of(c * mc + direction * me_half, me_half), me_half)
        x_cols[...] = x[:, at].T
        for g in range((embed + kvw) // 256):
            block = dot(x_cols[...], dqkv[:, g * 256:(g + 1) * 256])
            for i in range(per):
                h = g * per + i
                piece = block[:, i * hd:(i + 1) * hd]
                if h < heads:
                    part_w[direction, pl.ds(h, me_half, stride=heads), :] = piece
                else:
                    part_w[direction, pl.ds(h * me_half, me_half), :] = piece

    ws = wrow // 2

    def w_sub(direction, c, sub):
        return pl.ds(pl.multiple_of(w_rows(direction, c) + sub * ws, ws), ws)

    def rw_copy(direction, t, sub):
        piece = arena.at[w_sub(direction, rs_chunk(direction, t), sub)]
        return rcopy(piece, piece, rw_send.at[direction, t, sub], rw_recv.at[direction, t, sub], direction)

    def rw_tick(direction, t, sub):
        rows = w_sub(direction, rs_chunk(direction, t), sub)
        rw_copy(direction, t - 1, sub).wait_recv()
        arena[rows, :] = arena[rows, :] + part_w[direction, sub_rows(sub, ws), :]

    def gw_copy(direction, t, sub):
        piece = arena.at[w_sub(direction, ag_chunk(direction, t), sub)]
        return rcopy(piece, piece, gw_send.at[direction, t, sub], gw_recv.at[direction, t, sub], direction)

    def extra_w():
        return extra_copy(arena.at[pl.ds(w_rows(first, rs_chunk(first, 0)), wrow)], extra_wb, 3)

    def gift_w():
        return extra_copy(arena.at[pl.ds(w_rows(first, me), wrow)], gift_wb, 4)

    w_part(second, 0)
    pl.semaphore_wait(ready_sem, 2)
    arena[pl.ds(w_rows(second, rs_chunk(second, 0)), wrow), :] = part_w[second]
    for sub in (0, 1):
        rw_copy(second, 0, sub).start()
    w_part(first, 1)
    for sub in (0, 1):
        rw_tick(first, 1, sub)
        rw_copy(first, 1, sub).start()
    w_part(first, 0)
    arena[pl.ds(w_rows(first, rs_chunk(first, 0)), wrow), :] = part_w[first]
    extra_w().start()
    w_part(second, 1)
    arena[pl.ds(w_rows(second, rs_chunk(second, 1)), wrow), :] = part_w[second]
    for sub in (0, 1):
        rw_copy(second, 1, sub).start()
    for direction in order:
        w_part(direction, 2)

    def third_step(t, carry):
        wait_sends(rw_copy, t - 2)
        for sub in (0, 1):
            for direction in order:
                rw_tick(direction, t, sub)
                rw_copy(direction, t, sub).start()
        for direction in order:
            w_part(direction, t + 1)
        return carry

    extra_w().wait_send()
    lax.fori_loop(2, n - 1, third_step, 0)

    def dx_piece(i):
        at = pl.ds(pl.multiple_of(i * mc, mc), mc)
        x[:, at] = dot_nt(dqkv[...], wqkv[at, :]).astype(BF16)

    for sub in (0, 1):
        rw_tick(first, n - 1, sub)
        gw_copy(first, 0, sub).start()
    gift_w().start()
    extra_w().wait_recv()
    part_w[second] = part_w[second] + extra_wb[...]
    for sub in (0, 1):
        rw_tick(second, n - 1, sub)
        gw_copy(second, 0, sub).start()
    dx_piece(0)
    dx_piece(1)

    def fourth_step(t, carry):
        @pl.when(t <= 2)
        def _():
            wait_sends(rw_copy, n - 4 + t)

        for sub in (0, 1):
            for direction in order:
                gw_copy(direction, t - 1, sub).wait_recv()
                ag_send(gw_copy(direction, t, sub), direction, t)
        dx_piece(t + 1)
        return carry

    lax.fori_loop(1, n - 1, fourth_step, 0)

    go_copy(first, n - 2).wait_recv()
    gift_o().wait_recv()
    for sub in (0, 1):
        gw_copy(first, n - 2, sub).wait_recv()
    gift_w().wait_recv()

    def drain_all(t, c):
        def drain_gather(direction):
            go_copy(direction, t).wait_send()
            for sub in (0, 1):
                gw_copy(direction, t, sub).wait_send()

        drain_gather(second)

        @pl.when(t < n - 2)
        def _():
            drain_gather(first)

        return c

    lax.fori_loop(0, n - 1, drain_all, 0)
    for copy in (gift_o, gift_w):
        copy().wait_send()
    last = ag_chunk(second, n - 1)
    slot_o[second, last] = gift_ob[...]
    arena[pl.ds(w_rows(second, last), wrow), :] = gift_wb[...]


def store_kernel(n, heads, x, dy, slot_o, arena, y_hbm, dx_hbm, gq_hbm, gk_hbm, gv_hbm, go_hbm, sem_a, sem_b):
    eh, mc = slot_o.shape[2:]
    mh = mc // 2
    wrow = mh * (heads + 2)
    copies = [pltpu.make_async_copy(dy, y_hbm, sem_a.at[0]), pltpu.make_async_copy(x, dx_hbm, sem_a.at[1])]
    for c in range(n):
        for d in range(2):
            dst = go_hbm.at[pl.ds(d * eh, eh), pl.ds(c * mc, mc)]
            copies.append(pltpu.make_async_copy(slot_o.at[d, c], dst, sem_b.at[d, c, 0]))
            row = (d * n + c) * wrow
            start = c * mc + d * mh
            for k, (out, skip, rows) in enumerate(((gq_hbm, 0, heads), (gk_hbm, heads, 1), (gv_hbm, heads + 1, 1))):
                copies.append(pltpu.make_async_copy(
                    arena.at[pl.ds(row + skip * mh, rows * mh)],
                    out.at[pl.ds(start * rows, rows * mh)], sem_b.at[d, c, k + 1],
                ))
    for copy in copies:
        copy.start()
    for copy in copies:
        copy.wait()


def solution(mesh):
    n = mesh.shape["cp"]
    row_spec = P(("dp", "cp"), None)
    rep_spec = P(None, None, None)
    part_spec = P("dp", None, None)

    def device_layer(hidden, grad_out, w_query, w_key, w_value, w_out):
        tok, width = hidden.shape
        heads, hd = w_query.shape[1], w_query.shape[2]
        embed = heads * hd
        kvw = 2 * hd
        half = tok // 2
        cols = heads * half
        mc = width // n
        wrow = mc // 2 * (heads + 2)
        dma = lambda *shape: pltpu.SemaphoreType.DMA(shape)
        ring = dma(2, n - 1)
        split_ring = dma(2, n - 1, 2)
        arena_rows = max(4 * n * tok, 2 * n * wrow)
        state = pl.pallas_call(
            functools.partial(layer_kernel, n, heads),
            name="attention_layer",
            out_shape=[
                pltpu.VMEM((tok, width), BF16),
                pltpu.VMEM((tok, width), BF16),
                pltpu.VMEM((2, n, embed // 2, mc), F32),
                pltpu.VMEM((arena_rows, hd), F32),
            ],
            in_specs=[HBM] * 6,
            out_specs=[VMEM] * 4,
            scratch_shapes=[
                pltpu.VMEM((width, embed + kvw), BF16),
                pltpu.VMEM((embed, width), BF16),
                pltpu.VMEM((n, tok, kvw), BF16),
                pltpu.VMEM((2, cols, hd), BF16),
                pltpu.VMEM((2, hd, cols), BF16),
                pltpu.VMEM((2, cols, hd), BF16),
                pltpu.VMEM((2, hd, cols), BF16),
                pltpu.VMEM((tok, embed), BF16),
                pltpu.VMEM((embed, tok), BF16),
                pltpu.VMEM((2, hd, cols), F32),
                pltpu.VMEM((2, 1, cols), F32),
                pltpu.VMEM((2, 1, cols), F32),
                pltpu.VMEM((2, 1, cols), F32),
                pltpu.VMEM((tok, embed + kvw), BF16),
                pltpu.VMEM((2, embed // 2, mc), F32),
                pltpu.VMEM((2, wrow, hd), F32),
                pltpu.VMEM((mc // 2, tok), BF16),
                pltpu.VMEM((embed // 2, mc), F32),
                pltpu.VMEM((embed // 2, mc), F32),
                pltpu.VMEM((tok, hd), F32),
                pltpu.VMEM((wrow, hd), F32),
                pltpu.VMEM((wrow, hd), F32),
                dma(6),
                dma(2, n // 2), dma(2, n // 2),
                split_ring, split_ring, ring, ring, ring, ring, split_ring, split_ring, split_ring, split_ring,
                dma(5), dma(5),
                pltpu.SemaphoreType.REGULAR,
            ],
            compiler_params=pltpu.CompilerParams(
                collective_id=0, has_side_effects=True, vmem_limit_bytes=30 * 2 ** 20
            ),
        )(
            hidden, grad_out, w_query.reshape(width, embed), w_key.reshape(width, hd), w_value.reshape(width, hd),
            w_out.reshape(embed, width),
        )
        output, grad_hidden, gq, gk, gv, go = pl.pallas_call(
            functools.partial(store_kernel, n, heads),
            name="store_results",
            out_shape=[
                jax.ShapeDtypeStruct((tok, width), BF16),
                jax.ShapeDtypeStruct((tok, width), BF16),
                jax.ShapeDtypeStruct((width * heads, hd), F32),
                jax.ShapeDtypeStruct((width, hd), F32),
                jax.ShapeDtypeStruct((width, hd), F32),
                jax.ShapeDtypeStruct((embed, width), F32),
            ],
            in_specs=[VMEM] * 4,
            out_specs=[HBM] * 6,
            scratch_shapes=[dma(2), dma(2, n, 4)],
            compiler_params=pltpu.CompilerParams(vmem_limit_bytes=2 ** 20),
        )(*state)
        return (
            output,
            grad_hidden,
            gq.reshape(width, heads, hd),
            gk.reshape(width, 1, hd),
            gv.reshape(width, 1, hd),
            go.reshape(heads, hd, width),
        )

    return jax.shard_map(
        device_layer,
        mesh=mesh,
        in_specs=(row_spec, row_spec, rep_spec, rep_spec, rep_spec, rep_spec),
        out_specs=(row_spec, row_spec, part_spec, part_spec, part_spec, part_spec),
        check_vma=False,
    )
```

```python
import functools
import math

import jax
import jax.numpy as jnp
from jax import lax
from jax.experimental import pallas as pl
from jax.experimental.pallas import tpu as pltpu
from jax.sharding import PartitionSpec as P

F32 = jnp.float32
BF16 = jnp.bfloat16
MESH = pl.DeviceIdType.MESH
HBM = pl.BlockSpec(memory_space=pl.ANY)
VMEM = pl.BlockSpec(memory_space=pltpu.VMEM)


def dot(a, b):
    return jnp.dot(a, b, preferred_element_type=F32)


def dot_nt(a, b):
    return lax.dot_general(a, b, (((1,), (1,)), ((), ())), preferred_element_type=F32)


def layer_kernel(
    n, heads, x_hbm, dy_hbm, wq_hbm, wk_hbm, wv_hbm, wo_hbm,
    x, dy, slot_o, arena,
    wqkv, wo, kv, q_rows, q_cols, do_rows, do_cols, o_rows, o_cols,
    acc, m_state, l_state, delta, dqkv, part_o, part_w, x_cols, extra_ob, gift_ob, extra_kvb, extra_wb, gift_wb,
    in_sem, kv_send, kv_recv, ro_send, ro_recv, go_send, go_recv, rkv_send, rkv_recv,
    rw_send, rw_recv, gw_send, gw_recv, extra_send, extra_recv, ready_sem,
):
    tok, width = x.shape
    half = tok // 2
    embed = wo.shape[0]
    hd = embed // heads
    kvw = wqkv.shape[1] - embed
    mc = width // n
    me_half = mc // 2
    cols = heads * half
    scale = hd ** -0.5
    scale2 = scale * math.log2(math.e)
    me = lax.axis_index("cp")
    right = lax.rem(me + 1, n)
    left = lax.rem(me + n - 1, n)
    second = lax.rem(me, 2)
    first = 1 - second
    order = (first, second)

    def wrap(i):
        return lax.rem(i + 2 * n, n)

    def rcopy(src, dst, send, recv, direction):
        return pltpu.make_async_remote_copy(
            src_ref=src, dst_ref=dst, send_sem=send, recv_sem=recv,
            device_id={"cp": right + direction * (left - right)}, device_id_type=MESH,
        )

    def rs_chunk(direction, t):
        return wrap(me + (2 * direction - 1) * (t + 1))

    def ag_chunk(direction, t):
        return wrap(me + (2 * direction - 1) * t)

    loads = [
        pltpu.make_async_copy(x_hbm, x, in_sem.at[0]),
        pltpu.make_async_copy(wk_hbm, wqkv.at[:, pl.ds(embed, kvw // 2)], in_sem.at[1]),
        pltpu.make_async_copy(wv_hbm, wqkv.at[:, pl.ds(embed + kvw // 2, kvw // 2)], in_sem.at[2]),
        pltpu.make_async_copy(wq_hbm, wqkv.at[:, pl.ds(0, embed)], in_sem.at[3]),
        pltpu.make_async_copy(dy_hbm, dy, in_sem.at[4]),
        pltpu.make_async_copy(wo_hbm, wo, in_sem.at[5]),
    ]
    for load in loads[:3]:
        load.start()

    barrier = pltpu.get_barrier_semaphore()
    for device in (left, right):
        pl.semaphore_signal(barrier, inc=1, device_id={"cp": device}, device_id_type=MESH)

    for load in loads[:3]:
        load.wait()
    for load in loads[3:]:
        load.start()

    kv[me] = dot(x[...], wqkv[:, embed:]).astype(BF16)
    pl.semaphore_wait(barrier, 2)

    def kv_copy(direction, t, sub):
        piece = kv.at[ag_chunk(direction, t), pl.ds(pl.multiple_of(sub * half, half), half)]
        return rcopy(piece, piece, kv_send.at[direction, t, sub], kv_recv.at[direction, t, sub], direction)

    def kv_steps(direction):
        return n // 2 + direction * (n - 1 - 2 * (n // 2))

    def kv_tick(direction, t, sub):
        @pl.when(t < kv_steps(direction))
        def _():
            kv_copy(direction, t, sub).wait_recv()

            @pl.when(t + 1 < kv_steps(direction))
            def _():
                kv_copy(direction, t + 1, sub).start()

    def kv_step(t, u):
        kv_tick(first, t, u)
        kv_tick(second, t, 1 - u)

    for sub in (0, 1):
        kv_copy(first, 0, sub).start()
        kv_copy(second, 0, 1 - sub).start()

    def spread(block, rows_ref, cols_ref, h):
        for b in range(2):
            piece = block[b * half:(b + 1) * half]
            rows_ref[b, h * half:(h + 1) * half, :] = piece
            cols_ref[b, :, h * half:(h + 1) * half] = piece.T

    per = 256 // hd

    def project_q(g):
        block = dot(x[...], wqkv[:, g * 256:(g + 1) * 256]).astype(BF16)
        for i in range(per):
            spread(block[:, i * hd:(i + 1) * hd], q_rows, q_cols, g * per + i)

    def project_do(g):
        block = dot_nt(dy[...], wo[g * 256:(g + 1) * 256, :]).astype(BF16)
        for i in range(per):
            spread(block[:, i * hd:(i + 1) * hd], do_rows, do_cols, g * per + i)

    loads[3].wait()
    for g in range(embed // 256):
        project_q(g)
        kv_step(g // 2, g % 2)
    early = embed // 512

    m_state[...] = jnp.full(m_state.shape, -jnp.inf, F32)
    l_state[...] = jnp.zeros(l_state.shape, F32)
    acc[...] = jnp.zeros(acc.shape, F32)

    def diagonal():
        key_id = lax.broadcasted_iota(jnp.int32, (half, cols), 0)
        query_id = lax.rem(lax.broadcasted_iota(jnp.int32, (half, cols), 1), half)
        return key_id <= query_id

    def forward_unit(s, qb, kb, masked):
        keys = kv[s, pl.ds(kb * half, half), :hd]
        values_t = kv[s, pl.ds(kb * half, half), hd:].T
        sc = dot(keys, q_cols[qb])
        if masked:
            sc = jnp.where(diagonal(), sc, -jnp.inf)
        old = m_state[qb]
        new = jnp.maximum(old, jnp.max(sc, axis=0, keepdims=True) * scale2)
        fade = jnp.exp2(old - new)
        p = jnp.exp2(sc * scale2 - new)
        l_state[qb] = l_state[qb] * fade + jnp.sum(p, axis=0, keepdims=True)
        m_state[qb] = new
        acc[qb] = acc[qb] * fade + dot(values_t, p.astype(BF16))

    forward_unit(me, 1, 0, False)
    forward_unit(me, 0, 0, True)
    forward_unit(me, 1, 1, True)

    def unit_blocks(s, u):
        same = jnp.where(s < me, 0, 1)
        return jnp.where(u == 0, 1, same), jnp.where(u == 0, 0, same)

    def forward_step(j, carry):
        direction = first + lax.rem(j, 2) * (second - first)
        kv_step(j // 2 + early, lax.rem(j, 2))
        s = rs_chunk(direction, j // 2)

        def unit(u, c):
            qb, kb = unit_blocks(s, u)
            forward_unit(s, qb, kb, False)
            return c

        return lax.fori_loop(0, 2, unit, carry)

    lax.fori_loop(0, n - 1, forward_step, 0)

    for direction in (0, 1):
        def drain(t, c, direction=direction):
            for sub in (0, 1):
                kv_copy(direction, t, sub).wait_send()
            return c

        lax.fori_loop(0, kv_steps(direction), drain, 0)

    for b in range(2):
        for h in range(heads):
            lanes = slice(h * half, (h + 1) * half)
            total = l_state[b, :, lanes]
            out = (acc[b, :, lanes] / total).astype(BF16)
            o_cols[h * hd:(h + 1) * hd, b * half:(b + 1) * half] = out
            o_rows[b * half:(b + 1) * half, h * hd:(h + 1) * hd] = out.T
            m_state[b, :, lanes] = m_state[b, :, lanes] + jnp.log(total) * math.log2(math.e)

    eh = embed // 2

    es = eh // 2

    def sub_rows(sub, size):
        return pl.ds(pl.multiple_of(sub * size, size), size)

    def wo_part(direction, t, sub):
        at = pl.ds(pl.multiple_of(rs_chunk(direction, t) * mc, mc), mc)
        rows = pl.ds(pl.multiple_of(direction * eh + sub * es, es), es)
        part_o[direction, sub_rows(sub, es), :] = dot(o_cols[rows, :], dy[:, at])

    def ro_copy(direction, t, sub):
        piece = slot_o.at[direction, rs_chunk(direction, t), sub_rows(sub, es)]
        return rcopy(piece, piece, ro_send.at[direction, t, sub], ro_recv.at[direction, t, sub], direction)

    def wait_sends(copy, t):
        for sub in (0, 1):
            copy(second, t, sub).wait_send()

            @pl.when(t > 0)
            def _(sub=sub):
                copy(first, t, sub).wait_send()

    def ro_tick(direction, t, sub):
        c = rs_chunk(direction, t)
        rows = sub_rows(sub, es)
        ro_copy(direction, t - 1, sub).wait_recv()
        slot_o[direction, c, rows, :] = slot_o[direction, c, rows, :] + part_o[direction, rows, :]

    def ro_step(t, u):
        for direction, sub in ((first, u), (second, 1 - u)):
            ro_tick(direction, t, sub)
            ro_copy(direction, t, sub).start()
        for direction, sub in ((first, u), (second, 1 - u)):
            wo_part(direction, t + 1, sub)

    def extra_copy(src, dst, k):
        return rcopy(src, dst, extra_send.at[k], extra_recv.at[k], second)

    def extra_o():
        return extra_copy(slot_o.at[first, rs_chunk(first, 0)], extra_ob, 0)

    def gift_o():
        return extra_copy(slot_o.at[first, me], gift_ob, 1)

    loads[4].wait()
    for sub in (0, 1):
        wo_part(second, 0, sub)
        slot_o[second, rs_chunk(second, 0), sub_rows(sub, es), :] = part_o[second, sub_rows(sub, es), :]
        ro_copy(second, 0, sub).start()
    for sub in (0, 1):
        wo_part(first, 1, sub)
        ro_tick(first, 1, sub)
        ro_copy(first, 1, sub).start()
    for sub in (0, 1):
        wo_part(second, 1, sub)
        slot_o[second, rs_chunk(second, 1), sub_rows(sub, es), :] = part_o[second, sub_rows(sub, es), :]
        ro_copy(second, 1, sub).start()
    for sub in (0, 1):
        wo_part(first, 0, sub)
    slot_o[first, rs_chunk(first, 0)] = part_o[first]
    extra_o().start()
    for sub in (0, 1):
        for direction in order:
            wo_part(direction, 2, sub)

    loads[5].wait()
    for g in range(embed // 256):
        project_do(g)
        if g < 2:
            ro_step(2, g)
    for b in range(2):
        for h in range(heads):
            lanes = slice(h * half, (h + 1) * half)
            out = o_cols[h * hd:(h + 1) * hd, b * half:(b + 1) * half].astype(F32)
            delta[b, :, lanes] = jnp.sum(out * do_cols[b, :, lanes].astype(F32), axis=0, keepdims=True)

    part_kv0 = 0
    slot_kv0 = 2 * n * tok

    def kv_rows(base, direction, c):
        return pl.multiple_of(base + (direction * n + c) * tok, tok)

    acc[...] = jnp.zeros(acc.shape, F32)

    def backward_unit(s, qb, kb, masked, add):
        keys = kv[s, pl.ds(kb * half, half), :hd]
        values = kv[s, pl.ds(kb * half, half), hd:]
        sc = dot(keys, q_cols[qb])
        p = jnp.exp2(sc * scale2 - m_state[qb])
        if masked:
            p = jnp.where(diagonal(), p, 0.0)
        p = p.astype(BF16)
        dp = dot(values, do_cols[qb])
        ds = (p.astype(F32) * (dp - delta[qb])).astype(BF16)
        acc[qb] = acc[qb] + dot(keys.T, ds)
        for direction, lhs, rhs in ((0, ds, q_rows), (1, p, do_rows)):
            rows = pl.ds(pl.multiple_of(kv_rows(part_kv0, direction, s) + kb * half, half), half)
            g = dot(lhs, rhs[qb])
            arena[rows, :] = arena[rows, :] + g if add else g

    def zero_block(s, kb):
        for direction in (0, 1):
            rows = pl.ds(pl.multiple_of(kv_rows(part_kv0, direction, s) + kb * half, half), half)
            arena[rows, :] = jnp.zeros((half, hd), F32)

    wait_sends(ro_copy, 0)
    extra_o().wait_send()
    backward_unit(me, 1, 0, False, False)
    backward_unit(me, 0, 0, True, True)
    backward_unit(me, 1, 1, True, False)

    def backward_step(j, carry):
        s = wrap(me + j)

        t = j + 2

        @pl.when(t < n - 1)
        def _():
            wait_sends(ro_copy, t - 2)

        zero_block(s, 0)
        zero_block(s, 1)

        def unit(u, c):
            @pl.when(t < n - 1)
            def _():
                ro_step(t, u)

            qb, kb = unit_blocks(s, u)
            backward_unit(s, qb, kb, False, True)
            return c

        return lax.fori_loop(0, 2, unit, carry)

    lax.fori_loop(1, n, backward_step, 0)

    for b in range(2):
        for h in range(heads):
            g = (acc[b, :, h * half:(h + 1) * half] * scale).astype(BF16)
            dqkv[b * half:(b + 1) * half, h * hd:(h + 1) * hd] = g.T

    def rkv_copy(direction, t):
        rows = pl.ds(kv_rows(slot_kv0, direction, rs_chunk(direction, t)), tok)
        return rcopy(arena.at[rows], arena.at[rows], rkv_send.at[direction, t], rkv_recv.at[direction, t], direction)

    def rkv_add(direction, c):
        slot = pl.ds(kv_rows(slot_kv0, direction, c), tok)
        part = pl.ds(kv_rows(part_kv0, direction, c), tok)
        return arena[slot, :] + arena[part, :]

    def go_copy(direction, t):
        c = ag_chunk(direction, t)
        return rcopy(slot_o.at[direction, c], slot_o.at[direction, c],
                     go_send.at[direction, t], go_recv.at[direction, t], direction)

    def y_piece(i):
        at = pl.ds(pl.multiple_of(i * mc, mc), mc)
        dy[:, at] = dot(o_rows[...], wo[:, at]).astype(BF16)

    def extra_kv():
        return extra_copy(arena.at[pl.ds(kv_rows(part_kv0, first, rs_chunk(first, 0)), tok)], extra_kvb, 2)

    extra_kv().start()
    for t in (0, 1):
        c = rs_chunk(second, t)
        arena[pl.ds(kv_rows(slot_kv0, second, c), tok), :] = arena[pl.ds(kv_rows(part_kv0, second, c), tok), :]
        rkv_copy(second, t).start()
    c = rs_chunk(first, 1)
    rkv_copy(first, 0).wait_recv()
    arena[pl.ds(kv_rows(slot_kv0, first, c), tok), :] = rkv_add(first, c)
    rkv_copy(first, 1).start()
    for sub in (0, 1):
        ro_tick(first, n - 1, sub)
    go_copy(first, 0).start()
    gift_o().start()
    extra_o().wait_recv()
    part_o[second] = part_o[second] + extra_ob[...]
    for sub in (0, 1):
        ro_tick(second, n - 1, sub)
    go_copy(second, 0).start()
    y_piece(0)
    y_piece(1)

    def ag_send(copy, direction, t):
        @pl.when(jnp.logical_or(t < n - 2, direction == second))
        def _():
            copy.start()

    def second_step(t, carry):
        u = t + 1
        for direction in order:
            @pl.when(u < n - 1)
            def _(direction=direction):
                c = rs_chunk(direction, u)
                rkv_copy(direction, u - 1).wait_recv()
                arena[pl.ds(kv_rows(slot_kv0, direction, c), tok), :] = rkv_add(direction, c)
                rkv_copy(direction, u).start()

        @pl.when(t <= 2)
        def _():
            wait_sends(ro_copy, n - 4 + t)

        for direction in order:
            go_copy(direction, t - 1).wait_recv()
            ag_send(go_copy(direction, t), direction, t)
        y_piece(t + 1)
        return carry

    lax.fori_loop(1, n - 1, second_step, 0)

    extra_kv().wait_recv()
    mine = pl.ds(kv_rows(slot_kv0, second, me), tok)
    rkv_copy(second, n - 2).wait_recv()
    arena[mine, :] = arena[mine, :] + extra_kvb[...]
    rkv_copy(first, n - 2).wait_recv()
    for direction in (0, 1):
        g = rkv_add(direction, me)
        if direction == 0:
            g = g * scale
        dqkv[:, embed + direction * hd:embed + (direction + 1) * hd] = g.astype(BF16)

    def drain_kv(t, c):
        rkv_copy(second, t).wait_send()

        @pl.when(t > 0)
        def _():
            rkv_copy(first, t).wait_send()

        return c

    lax.fori_loop(0, n - 1, drain_kv, 0)
    extra_kv().wait_send()
    for device in (left, right):
        pl.semaphore_signal(ready_sem, inc=1, device_id={"cp": device}, device_id_type=MESH)

    wrow = me_half * (heads + 2)

    def w_rows(direction, c):
        return pl.multiple_of((direction * n + c) * wrow, wrow)

    def w_part(direction, t):
        c = rs_chunk(direction, t)
        at = pl.ds(pl.multiple_of(c * mc + direction * me_half, me_half), me_half)
        x_cols[...] = x[:, at].T
        for g in range((embed + kvw) // 256):
            block = dot(x_cols[...], dqkv[:, g * 256:(g + 1) * 256])
            for i in range(per):
                h = g * per + i
                piece = block[:, i * hd:(i + 1) * hd]
                if h < heads:
                    part_w[direction, pl.ds(h, me_half, stride=heads), :] = piece
                else:
                    part_w[direction, pl.ds(h * me_half, me_half), :] = piece

    ws = wrow // 2

    def w_sub(direction, c, sub):
        return pl.ds(pl.multiple_of(w_rows(direction, c) + sub * ws, ws), ws)

    def rw_copy(direction, t, sub):
        piece = arena.at[w_sub(direction, rs_chunk(direction, t), sub)]
        return rcopy(piece, piece, rw_send.at[direction, t, sub], rw_recv.at[direction, t, sub], direction)

    def rw_tick(direction, t, sub):
        rows = w_sub(direction, rs_chunk(direction, t), sub)
        rw_copy(direction, t - 1, sub).wait_recv()
        arena[rows, :] = arena[rows, :] + part_w[direction, sub_rows(sub, ws), :]

    def gw_copy(direction, t, sub):
        piece = arena.at[w_sub(direction, ag_chunk(direction, t), sub)]
        return rcopy(piece, piece, gw_send.at[direction, t, sub], gw_recv.at[direction, t, sub], direction)

    def extra_w():
        return extra_copy(arena.at[pl.ds(w_rows(first, rs_chunk(first, 0)), wrow)], extra_wb, 3)

    def gift_w():
        return extra_copy(arena.at[pl.ds(w_rows(first, me), wrow)], gift_wb, 4)

    w_part(second, 0)
    pl.semaphore_wait(ready_sem, 2)
    arena[pl.ds(w_rows(second, rs_chunk(second, 0)), wrow), :] = part_w[second]
    for sub in (0, 1):
        rw_copy(second, 0, sub).start()
    w_part(first, 1)
    for sub in (0, 1):
        rw_tick(first, 1, sub)
        rw_copy(first, 1, sub).start()
    w_part(first, 0)
    arena[pl.ds(w_rows(first, rs_chunk(first, 0)), wrow), :] = part_w[first]
    extra_w().start()
    w_part(second, 1)
    arena[pl.ds(w_rows(second, rs_chunk(second, 1)), wrow), :] = part_w[second]
    for sub in (0, 1):
        rw_copy(second, 1, sub).start()
    for direction in order:
        w_part(direction, 2)

    def third_step(t, carry):
        wait_sends(rw_copy, t - 2)
        for sub in (0, 1):
            for direction in order:
                rw_tick(direction, t, sub)
                rw_copy(direction, t, sub).start()
        for direction in order:
            w_part(direction, t + 1)
        return carry

    extra_w().wait_send()
    lax.fori_loop(2, n - 1, third_step, 0)

    def dx_piece(i):
        at = pl.ds(pl.multiple_of(i * mc, mc), mc)
        x[:, at] = dot_nt(dqkv[...], wqkv[at, :]).astype(BF16)

    for sub in (0, 1):
        rw_tick(first, n - 1, sub)
        gw_copy(first, 0, sub).start()
    gift_w().start()
    extra_w().wait_recv()
    part_w[second] = part_w[second] + extra_wb[...]
    for sub in (0, 1):
        rw_tick(second, n - 1, sub)
        gw_copy(second, 0, sub).start()
    dx_piece(0)
    dx_piece(1)

    def fourth_step(t, carry):
        @pl.when(t <= 2)
        def _():
            wait_sends(rw_copy, n - 4 + t)

        for sub in (0, 1):
            for direction in order:
                gw_copy(direction, t - 1, sub).wait_recv()
                ag_send(gw_copy(direction, t, sub), direction, t)
        dx_piece(t + 1)
        return carry

    lax.fori_loop(1, n - 1, fourth_step, 0)

    go_copy(first, n - 2).wait_recv()
    gift_o().wait_recv()
    for sub in (0, 1):
        gw_copy(first, n - 2, sub).wait_recv()
    gift_w().wait_recv()

    def drain_all(t, c):
        def drain_gather(direction):
            go_copy(direction, t).wait_send()
            for sub in (0, 1):
                gw_copy(direction, t, sub).wait_send()

        drain_gather(second)

        @pl.when(t < n - 2)
        def _():
            drain_gather(first)

        return c

    lax.fori_loop(0, n - 1, drain_all, 0)
    for copy in (gift_o, gift_w):
        copy().wait_send()
    last = ag_chunk(second, n - 1)
    slot_o[second, last] = gift_ob[...]
    arena[pl.ds(w_rows(second, last), wrow), :] = gift_wb[...]


def store_kernel(n, heads, x, dy, slot_o, arena, y_hbm, dx_hbm, gq_hbm, gk_hbm, gv_hbm, go_hbm, sem_a, sem_b):
    eh, mc = slot_o.shape[2:]
    mh = mc // 2
    wrow = mh * (heads + 2)
    copies = [pltpu.make_async_copy(dy, y_hbm, sem_a.at[0]), pltpu.make_async_copy(x, dx_hbm, sem_a.at[1])]
    for c in range(n):
        for d in range(2):
            dst = go_hbm.at[pl.ds(d * eh, eh), pl.ds(c * mc, mc)]
            copies.append(pltpu.make_async_copy(slot_o.at[d, c], dst, sem_b.at[d, c, 0]))
            row = (d * n + c) * wrow
            start = c * mc + d * mh
            for k, (out, skip, rows) in enumerate(((gq_hbm, 0, heads), (gk_hbm, heads, 1), (gv_hbm, heads + 1, 1))):
                copies.append(pltpu.make_async_copy(
                    arena.at[pl.ds(row + skip * mh, rows * mh)],
                    out.at[pl.ds(start * rows, rows * mh)], sem_b.at[d, c, k + 1],
                ))
    for copy in copies:
        copy.start()
    for copy in copies:
        copy.wait()


def solution(mesh):
    n = mesh.shape["cp"]
    row_spec = P(("dp", "cp"), None)
    rep_spec = P(None, None, None)
    part_spec = P("dp", None, None)

    def device_layer(hidden, grad_out, w_query, w_key, w_value, w_out):
        tok, width = hidden.shape
        heads, hd = w_query.shape[1], w_query.shape[2]
        embed = heads * hd
        kvw = 2 * hd
        half = tok // 2
        cols = heads * half
        mc = width // n
        wrow = mc // 2 * (heads + 2)
        dma = lambda *shape: pltpu.SemaphoreType.DMA(shape)
        ring = dma(2, n - 1)
        split_ring = dma(2, n - 1, 2)
        arena_rows = max(4 * n * tok, 2 * n * wrow)
        state = pl.pallas_call(
            functools.partial(layer_kernel, n, heads),
            name="attention_layer",
            out_shape=[
                pltpu.VMEM((tok, width), BF16),
                pltpu.VMEM((tok, width), BF16),
                pltpu.VMEM((2, n, embed // 2, mc), F32),
                pltpu.VMEM((arena_rows, hd), F32),
            ],
            in_specs=[HBM] * 6,
            out_specs=[VMEM] * 4,
            scratch_shapes=[
                pltpu.VMEM((width, embed + kvw), BF16),
                pltpu.VMEM((embed, width), BF16),
                pltpu.VMEM((n, tok, kvw), BF16),
                pltpu.VMEM((2, cols, hd), BF16),
                pltpu.VMEM((2, hd, cols), BF16),
                pltpu.VMEM((2, cols, hd), BF16),
                pltpu.VMEM((2, hd, cols), BF16),
                pltpu.VMEM((tok, embed), BF16),
                pltpu.VMEM((embed, tok), BF16),
                pltpu.VMEM((2, hd, cols), F32),
                pltpu.VMEM((2, 1, cols), F32),
                pltpu.VMEM((2, 1, cols), F32),
                pltpu.VMEM((2, 1, cols), F32),
                pltpu.VMEM((tok, embed + kvw), BF16),
                pltpu.VMEM((2, embed // 2, mc), F32),
                pltpu.VMEM((2, wrow, hd), F32),
                pltpu.VMEM((mc // 2, tok), BF16),
                pltpu.VMEM((embed // 2, mc), F32),
                pltpu.VMEM((embed // 2, mc), F32),
                pltpu.VMEM((tok, hd), F32),
                pltpu.VMEM((wrow, hd), F32),
                pltpu.VMEM((wrow, hd), F32),
                dma(6),
                dma(2, n // 2, 2), dma(2, n // 2, 2),
                split_ring, split_ring, ring, ring, ring, ring, split_ring, split_ring, split_ring, split_ring,
                dma(5), dma(5),
                pltpu.SemaphoreType.REGULAR,
            ],
            compiler_params=pltpu.CompilerParams(
                collective_id=0, has_side_effects=True, vmem_limit_bytes=30 * 2 ** 20
            ),
        )(
            hidden, grad_out, w_query.reshape(width, embed), w_key.reshape(width, hd), w_value.reshape(width, hd),
            w_out.reshape(embed, width),
        )
        output, grad_hidden, gq, gk, gv, go = pl.pallas_call(
            functools.partial(store_kernel, n, heads),
            name="store_results",
            out_shape=[
                jax.ShapeDtypeStruct((tok, width), BF16),
                jax.ShapeDtypeStruct((tok, width), BF16),
                jax.ShapeDtypeStruct((width * heads, hd), F32),
                jax.ShapeDtypeStruct((width, hd), F32),
                jax.ShapeDtypeStruct((width, hd), F32),
                jax.ShapeDtypeStruct((embed, width), F32),
            ],
            in_specs=[VMEM] * 4,
            out_specs=[HBM] * 6,
            scratch_shapes=[dma(2), dma(2, n, 4)],
            compiler_params=pltpu.CompilerParams(vmem_limit_bytes=2 ** 20),
        )(*state)
        return (
            output,
            grad_hidden,
            gq.reshape(width, heads, hd),
            gk.reshape(width, 1, hd),
            gv.reshape(width, 1, hd),
            go.reshape(heads, hd, width),
        )

    return jax.shard_map(
        device_layer,
        mesh=mesh,
        in_specs=(row_spec, row_spec, rep_spec, rep_spec, rep_spec, rep_spec),
        out_specs=(row_spec, row_spec, part_spec, part_spec, part_spec, part_spec),
        check_vma=False,
    )
```

```python
import functools
import math

import jax
import jax.numpy as jnp
from jax import lax
from jax.experimental import pallas as pl
from jax.experimental.pallas import tpu as pltpu
from jax.sharding import PartitionSpec as P

F32 = jnp.float32
BF16 = jnp.bfloat16
MESH = pl.DeviceIdType.MESH
HBM = pl.BlockSpec(memory_space=pl.ANY)
VMEM = pl.BlockSpec(memory_space=pltpu.VMEM)


def dot(a, b):
    return jnp.dot(a, b, preferred_element_type=F32)


def dot_nt(a, b):
    return lax.dot_general(a, b, (((1,), (1,)), ((), ())), preferred_element_type=F32)


def layer_kernel(
    n, heads, x_hbm, dy_hbm, wq_hbm, wk_hbm, wv_hbm, wo_hbm,
    x, dy, slot_o, arena,
    wqkv, wo, kv, q_rows, q_cols, do_rows, do_cols, o_rows, o_cols,
    acc, m_state, l_state, delta, dqkv, part_o, part_w, x_cols, extra_ob, gift_ob, extra_kvb, extra_wb, gift_wb,
    in_sem, kv_send, kv_recv, ro_send, ro_recv, go_send, go_recv, rkv_send, rkv_recv,
    rw_send, rw_recv, gw_send, gw_recv, extra_send, extra_recv, ready_sem,
):
    tok, width = x.shape
    half = tok // 2
    embed = wo.shape[0]
    hd = embed // heads
    kvw = wqkv.shape[1] - embed
    mc = width // n
    me_half = mc // 2
    cols = heads * half
    scale = hd ** -0.5
    scale2 = scale * math.log2(math.e)
    me = lax.axis_index("cp")
    right = lax.rem(me + 1, n)
    left = lax.rem(me + n - 1, n)
    second = lax.rem(me, 2)
    first = 1 - second
    order = (first, second)

    def wrap(i):
        return lax.rem(i + 2 * n, n)

    def rcopy(src, dst, send, recv, direction):
        return pltpu.make_async_remote_copy(
            src_ref=src, dst_ref=dst, send_sem=send, recv_sem=recv,
            device_id={"cp": right + direction * (left - right)}, device_id_type=MESH,
        )

    def rs_chunk(direction, t):
        return wrap(me + (2 * direction - 1) * (t + 1))

    def ag_chunk(direction, t):
        return wrap(me + (2 * direction - 1) * t)

    loads = [
        pltpu.make_async_copy(x_hbm, x, in_sem.at[0]),
        pltpu.make_async_copy(wk_hbm, wqkv.at[:, pl.ds(embed, kvw // 2)], in_sem.at[1]),
        pltpu.make_async_copy(wv_hbm, wqkv.at[:, pl.ds(embed + kvw // 2, kvw // 2)], in_sem.at[2]),
        pltpu.make_async_copy(wq_hbm, wqkv.at[:, pl.ds(0, embed)], in_sem.at[3]),
        pltpu.make_async_copy(dy_hbm, dy, in_sem.at[4]),
        pltpu.make_async_copy(wo_hbm, wo, in_sem.at[5]),
    ]
    for load in loads[:3]:
        load.start()

    barrier = pltpu.get_barrier_semaphore()
    for device in (left, right):
        pl.semaphore_signal(barrier, inc=1, device_id={"cp": device}, device_id_type=MESH)

    for load in loads[:3]:
        load.wait()
    for load in loads[3:]:
        load.start()

    kv[me] = dot(x[...], wqkv[:, embed:]).astype(BF16)
    pl.semaphore_wait(barrier, 2)

    def kv_copy(direction, t):
        c = ag_chunk(direction, t)
        return rcopy(kv.at[c], kv.at[c], kv_send.at[direction, t], kv_recv.at[direction, t], direction)

    def kv_steps(direction):
        return n // 2 + direction * (n - 1 - 2 * (n // 2))

    def kv_tick(direction, t):
        @pl.when(t < kv_steps(direction))
        def _():
            kv_copy(direction, t).wait_recv()

            @pl.when(t + 1 < kv_steps(direction))
            def _():
                kv_copy(direction, t + 1).start()

    for direction in order:
        kv_copy(direction, 0).start()

    def spread(block, rows_ref, cols_ref, h):
        for b in range(2):
            piece = block[b * half:(b + 1) * half]
            rows_ref[b, h * half:(h + 1) * half, :] = piece
            cols_ref[b, :, h * half:(h + 1) * half] = piece.T

    per = 256 // hd

    def project_q(g):
        block = dot(x[...], wqkv[:, g * 256:(g + 1) * 256]).astype(BF16)
        for i in range(per):
            spread(block[:, i * hd:(i + 1) * hd], q_rows, q_cols, g * per + i)

    def project_do(g):
        block = dot_nt(dy[...], wo[g * 256:(g + 1) * 256, :]).astype(BF16)
        for i in range(per):
            spread(block[:, i * hd:(i + 1) * hd], do_rows, do_cols, g * per + i)

    loads[3].wait()
    for g in range(embed // 256):
        project_q(g)
        kv_tick(order[g % 2], g // 2)
    early = embed // 512

    m_state[...] = jnp.full(m_state.shape, -jnp.inf, F32)
    l_state[...] = jnp.zeros(l_state.shape, F32)
    acc[...] = jnp.zeros(acc.shape, F32)

    def diagonal():
        key_id = lax.broadcasted_iota(jnp.int32, (half, cols), 0)
        query_id = lax.rem(lax.broadcasted_iota(jnp.int32, (half, cols), 1), half)
        return key_id <= query_id

    def forward_unit(s, qb, kb, masked):
        keys = kv[s, pl.ds(kb * half, half), :hd]
        values_t = kv[s, pl.ds(kb * half, half), hd:].T
        sc = dot(keys, q_cols[qb])
        if masked:
            sc = jnp.where(diagonal(), sc, -jnp.inf)
        old = m_state[qb]
        new = jnp.maximum(old, jnp.max(sc, axis=0, keepdims=True) * scale2)
        fade = jnp.exp2(old - new)
        p = jnp.exp2(sc * scale2 - new)
        l_state[qb] = l_state[qb] * fade + jnp.sum(p, axis=0, keepdims=True)
        m_state[qb] = new
        acc[qb] = acc[qb] * fade + dot(values_t, p.astype(BF16))

    forward_unit(me, 1, 0, False)
    forward_unit(me, 0, 0, True)
    forward_unit(me, 1, 1, True)

    def unit_blocks(s, u):
        same = jnp.where(s < me, 0, 1)
        return jnp.where(u == 0, 1, same), jnp.where(u == 0, 0, same)

    def forward_step(j, carry):
        direction = first + lax.rem(j, 2) * (second - first)
        kv_tick(direction, j // 2 + early)
        s = rs_chunk(direction, j // 2)

        def unit(u, c):
            qb, kb = unit_blocks(s, u)
            forward_unit(s, qb, kb, False)
            return c

        return lax.fori_loop(0, 2, unit, carry)

    lax.fori_loop(0, n - 1, forward_step, 0)

    for direction in (0, 1):
        def drain(t, c, direction=direction):
            kv_copy(direction, t).wait_send()
            return c

        lax.fori_loop(0, kv_steps(direction), drain, 0)

    for b in range(2):
        for h in range(heads):
            lanes = slice(h * half, (h + 1) * half)
            total = l_state[b, :, lanes]
            out = (acc[b, :, lanes] / total).astype(BF16)
            o_cols[h * hd:(h + 1) * hd, b * half:(b + 1) * half] = out
            o_rows[b * half:(b + 1) * half, h * hd:(h + 1) * hd] = out.T
            m_state[b, :, lanes] = m_state[b, :, lanes] + jnp.log(total) * math.log2(math.e)

    eh = embed // 2

    es = eh // 2

    def sub_rows(sub, size):
        return pl.ds(pl.multiple_of(sub * size, size), size)

    def wo_part(direction, t, sub):
        at = pl.ds(pl.multiple_of(rs_chunk(direction, t) * mc, mc), mc)
        rows = pl.ds(pl.multiple_of(direction * eh + sub * es, es), es)
        part_o[direction, sub_rows(sub, es), :] = dot(o_cols[rows, :], dy[:, at])

    def ro_copy(direction, t, sub):
        piece = slot_o.at[direction, rs_chunk(direction, t), sub_rows(sub, es)]
        return rcopy(piece, piece, ro_send.at[direction, t, sub], ro_recv.at[direction, t, sub], direction)

    def wait_sends(copy, t):
        for sub in (0, 1):
            copy(second, t, sub).wait_send()

            @pl.when(t > 0)
            def _(sub=sub):
                copy(first, t, sub).wait_send()

    def ro_tick(direction, t, sub):
        c = rs_chunk(direction, t)
        rows = sub_rows(sub, es)
        ro_copy(direction, t - 1, sub).wait_recv()
        slot_o[direction, c, rows, :] = slot_o[direction, c, rows, :] + part_o[direction, rows, :]

    def ro_send_on(direction, t, sub):
        ro_tick(direction, t, sub)
        ro_copy(direction, t, sub).start()

    def ro_step(t, u):
        pair = ((first, t, u), (second, t - 1 + u, 1 - u))
        for direction, at, sub in pair:
            ro_send_on(direction, at, sub)
        for direction, at, sub in pair:
            wo_part(direction, at + 1, sub)

    def extra_copy(src, dst, k):
        return rcopy(src, dst, extra_send.at[k], extra_recv.at[k], second)

    def extra_o():
        return extra_copy(slot_o.at[first, rs_chunk(first, 0)], extra_ob, 0)

    def gift_o():
        return extra_copy(slot_o.at[first, me], gift_ob, 1)

    loads[4].wait()
    for sub in (0, 1):
        wo_part(second, 0, sub)
        slot_o[second, rs_chunk(second, 0), sub_rows(sub, es), :] = part_o[second, sub_rows(sub, es), :]
        ro_copy(second, 0, sub).start()
    for sub in (0, 1):
        wo_part(first, 1, sub)
        ro_tick(first, 1, sub)
        ro_copy(first, 1, sub).start()
    for sub in (0, 1):
        wo_part(second, 1, sub)
        slot_o[second, rs_chunk(second, 1), sub_rows(sub, es), :] = part_o[second, sub_rows(sub, es), :]
        ro_copy(second, 1, sub).start()
    for sub in (0, 1):
        wo_part(first, 0, sub)
    slot_o[first, rs_chunk(first, 0)] = part_o[first]
    extra_o().start()
    for sub in (0, 1):
        for direction in order:
            wo_part(direction, 2, sub)

    loads[5].wait()
    for g in range(embed // 256):
        project_do(g)
        if g == 0:
            ro_send_on(first, 2, 0)
            wo_part(first, 3, 0)
        if g == 1:
            ro_step(2, 1)
    for b in range(2):
        for h in range(heads):
            lanes = slice(h * half, (h + 1) * half)
            out = o_cols[h * hd:(h + 1) * hd, b * half:(b + 1) * half].astype(F32)
            delta[b, :, lanes] = jnp.sum(out * do_cols[b, :, lanes].astype(F32), axis=0, keepdims=True)

    part_kv0 = 0
    slot_kv0 = 2 * n * tok

    def kv_rows(base, direction, c):
        return pl.multiple_of(base + (direction * n + c) * tok, tok)

    acc[...] = jnp.zeros(acc.shape, F32)

    def backward_unit(s, qb, kb, masked, add):
        keys = kv[s, pl.ds(kb * half, half), :hd]
        values = kv[s, pl.ds(kb * half, half), hd:]
        sc = dot(keys, q_cols[qb])
        p = jnp.exp2(sc * scale2 - m_state[qb])
        if masked:
            p = jnp.where(diagonal(), p, 0.0)
        p = p.astype(BF16)
        dp = dot(values, do_cols[qb])
        ds = (p.astype(F32) * (dp - delta[qb])).astype(BF16)
        acc[qb] = acc[qb] + dot(keys.T, ds)
        for direction, lhs, rhs in ((0, ds, q_rows), (1, p, do_rows)):
            rows = pl.ds(pl.multiple_of(kv_rows(part_kv0, direction, s) + kb * half, half), half)
            g = dot(lhs, rhs[qb])
            arena[rows, :] = arena[rows, :] + g if add else g

    def zero_block(s, kb):
        for direction in (0, 1):
            rows = pl.ds(pl.multiple_of(kv_rows(part_kv0, direction, s) + kb * half, half), half)
            arena[rows, :] = jnp.zeros((half, hd), F32)

    wait_sends(ro_copy, 0)
    extra_o().wait_send()
    backward_unit(me, 1, 0, False, False)
    backward_unit(me, 0, 0, True, True)
    backward_unit(me, 1, 1, True, False)

    def backward_step(j, carry):
        s = wrap(me + j)

        t = j + 2

        @pl.when(t < n - 1)
        def _():
            wait_sends(ro_copy, t - 2)

        zero_block(s, 0)
        zero_block(s, 1)

        def unit(u, c):
            @pl.when(t < n - 1)
            def _():
                ro_step(t, u)

            @pl.when(jnp.logical_and(t == n - 1, u == 0))
            def _():
                ro_send_on(second, n - 2, 1)
                wo_part(second, n - 1, 1)

            qb, kb = unit_blocks(s, u)
            backward_unit(s, qb, kb, False, True)
            return c

        return lax.fori_loop(0, 2, unit, carry)

    lax.fori_loop(1, n, backward_step, 0)

    for b in range(2):
        for h in range(heads):
            g = (acc[b, :, h * half:(h + 1) * half] * scale).astype(BF16)
            dqkv[b * half:(b + 1) * half, h * hd:(h + 1) * hd] = g.T

    def rkv_copy(direction, t):
        rows = pl.ds(kv_rows(slot_kv0, direction, rs_chunk(direction, t)), tok)
        return rcopy(arena.at[rows], arena.at[rows], rkv_send.at[direction, t], rkv_recv.at[direction, t], direction)

    def rkv_add(direction, c):
        slot = pl.ds(kv_rows(slot_kv0, direction, c), tok)
        part = pl.ds(kv_rows(part_kv0, direction, c), tok)
        return arena[slot, :] + arena[part, :]

    def go_copy(direction, t):
        c = ag_chunk(direction, t)
        return rcopy(slot_o.at[direction, c], slot_o.at[direction, c],
                     go_send.at[direction, t], go_recv.at[direction, t], direction)

    def y_piece(i):
        at = pl.ds(pl.multiple_of(i * mc, mc), mc)
        dy[:, at] = dot(o_rows[...], wo[:, at]).astype(BF16)

    def extra_kv():
        return extra_copy(arena.at[pl.ds(kv_rows(part_kv0, first, rs_chunk(first, 0)), tok)], extra_kvb, 2)

    extra_kv().start()
    for t in (0, 1):
        c = rs_chunk(second, t)
        arena[pl.ds(kv_rows(slot_kv0, second, c), tok), :] = arena[pl.ds(kv_rows(part_kv0, second, c), tok), :]
        rkv_copy(second, t).start()
    c = rs_chunk(first, 1)
    rkv_copy(first, 0).wait_recv()
    arena[pl.ds(kv_rows(slot_kv0, first, c), tok), :] = rkv_add(first, c)
    rkv_copy(first, 1).start()
    for sub in (0, 1):
        ro_tick(first, n - 1, sub)
    go_copy(first, 0).start()
    gift_o().start()
    extra_o().wait_recv()
    part_o[second] = part_o[second] + extra_ob[...]
    for sub in (0, 1):
        ro_tick(second, n - 1, sub)
    go_copy(second, 0).start()
    y_piece(0)
    y_piece(1)

    def ag_send(copy, direction, t):
        @pl.when(jnp.logical_or(t < n - 2, direction == second))
        def _():
            copy.start()

    def second_step(t, carry):
        u = t + 1
        for direction in order:
            @pl.when(u < n - 1)
            def _(direction=direction):
                c = rs_chunk(direction, u)
                rkv_copy(direction, u - 1).wait_recv()
                arena[pl.ds(kv_rows(slot_kv0, direction, c), tok), :] = rkv_add(direction, c)
                rkv_copy(direction, u).start()

        @pl.when(t <= 2)
        def _():
            wait_sends(ro_copy, n - 4 + t)

        for direction in order:
            go_copy(direction, t - 1).wait_recv()
            ag_send(go_copy(direction, t), direction, t)
        y_piece(t + 1)
        return carry

    lax.fori_loop(1, n - 1, second_step, 0)

    extra_kv().wait_recv()
    mine = pl.ds(kv_rows(slot_kv0, second, me), tok)
    rkv_copy(second, n - 2).wait_recv()
    arena[mine, :] = arena[mine, :] + extra_kvb[...]
    rkv_copy(first, n - 2).wait_recv()
    for direction in (0, 1):
        g = rkv_add(direction, me)
        if direction == 0:
            g = g * scale
        dqkv[:, embed + direction * hd:embed + (direction + 1) * hd] = g.astype(BF16)

    def drain_kv(t, c):
        rkv_copy(second, t).wait_send()

        @pl.when(t > 0)
        def _():
            rkv_copy(first, t).wait_send()

        return c

    lax.fori_loop(0, n - 1, drain_kv, 0)
    extra_kv().wait_send()
    for device in (left, right):
        pl.semaphore_signal(ready_sem, inc=1, device_id={"cp": device}, device_id_type=MESH)

    wrow = me_half * (heads + 2)

    def w_rows(direction, c):
        return pl.multiple_of((direction * n + c) * wrow, wrow)

    def w_part(direction, t):
        c = rs_chunk(direction, t)
        at = pl.ds(pl.multiple_of(c * mc + direction * me_half, me_half), me_half)
        x_cols[...] = x[:, at].T
        for g in range((embed + kvw) // 256):
            block = dot(x_cols[...], dqkv[:, g * 256:(g + 1) * 256])
            for i in range(per):
                h = g * per + i
                piece = block[:, i * hd:(i + 1) * hd]
                if h < heads:
                    part_w[direction, pl.ds(h, me_half, stride=heads), :] = piece
                else:
                    part_w[direction, pl.ds(h * me_half, me_half), :] = piece

    ws = wrow // 2

    def w_sub(direction, c, sub):
        return pl.ds(pl.multiple_of(w_rows(direction, c) + sub * ws, ws), ws)

    def rw_copy(direction, t, sub):
        piece = arena.at[w_sub(direction, rs_chunk(direction, t), sub)]
        return rcopy(piece, piece, rw_send.at[direction, t, sub], rw_recv.at[direction, t, sub], direction)

    def rw_tick(direction, t, sub):
        rows = w_sub(direction, rs_chunk(direction, t), sub)
        rw_copy(direction, t - 1, sub).wait_recv()
        arena[rows, :] = arena[rows, :] + part_w[direction, sub_rows(sub, ws), :]

    def gw_copy(direction, t, sub):
        piece = arena.at[w_sub(direction, ag_chunk(direction, t), sub)]
        return rcopy(piece, piece, gw_send.at[direction, t, sub], gw_recv.at[direction, t, sub], direction)

    def extra_w():
        return extra_copy(arena.at[pl.ds(w_rows(first, rs_chunk(first, 0)), wrow)], extra_wb, 3)

    def gift_w():
        return extra_copy(arena.at[pl.ds(w_rows(first, me), wrow)], gift_wb, 4)

    w_part(second, 0)
    pl.semaphore_wait(ready_sem, 2)
    arena[pl.ds(w_rows(second, rs_chunk(second, 0)), wrow), :] = part_w[second]
    for sub in (0, 1):
        rw_copy(second, 0, sub).start()
    w_part(first, 1)
    for sub in (0, 1):
        rw_tick(first, 1, sub)
        rw_copy(first, 1, sub).start()
    w_part(first, 0)
    arena[pl.ds(w_rows(first, rs_chunk(first, 0)), wrow), :] = part_w[first]
    extra_w().start()
    w_part(second, 1)
    arena[pl.ds(w_rows(second, rs_chunk(second, 1)), wrow), :] = part_w[second]
    for sub in (0, 1):
        rw_copy(second, 1, sub).start()
    for direction in order:
        w_part(direction, 2)

    def third_step(t, carry):
        wait_sends(rw_copy, t - 2)
        for sub in (0, 1):
            for direction in order:
                rw_tick(direction, t, sub)
                rw_copy(direction, t, sub).start()
        for direction in order:
            w_part(direction, t + 1)
        return carry

    extra_w().wait_send()
    lax.fori_loop(2, n - 1, third_step, 0)

    def dx_piece(i):
        at = pl.ds(pl.multiple_of(i * mc, mc), mc)
        x[:, at] = dot_nt(dqkv[...], wqkv[at, :]).astype(BF16)

    for sub in (0, 1):
        rw_tick(first, n - 1, sub)
        gw_copy(first, 0, sub).start()
    gift_w().start()
    extra_w().wait_recv()
    part_w[second] = part_w[second] + extra_wb[...]
    for sub in (0, 1):
        rw_tick(second, n - 1, sub)
        gw_copy(second, 0, sub).start()
    dx_piece(0)
    dx_piece(1)

    def fourth_step(t, carry):
        @pl.when(t <= 2)
        def _():
            wait_sends(rw_copy, n - 4 + t)

        for sub in (0, 1):
            for direction in order:
                gw_copy(direction, t - 1, sub).wait_recv()
                ag_send(gw_copy(direction, t, sub), direction, t)
        dx_piece(t + 1)
        return carry

    lax.fori_loop(1, n - 1, fourth_step, 0)

    go_copy(first, n - 2).wait_recv()
    gift_o().wait_recv()
    for sub in (0, 1):
        gw_copy(first, n - 2, sub).wait_recv()
    gift_w().wait_recv()

    def drain_all(t, c):
        def drain_gather(direction):
            go_copy(direction, t).wait_send()
            for sub in (0, 1):
                gw_copy(direction, t, sub).wait_send()

        drain_gather(second)

        @pl.when(t < n - 2)
        def _():
            drain_gather(first)

        return c

    lax.fori_loop(0, n - 1, drain_all, 0)
    for copy in (gift_o, gift_w):
        copy().wait_send()
    last = ag_chunk(second, n - 1)
    slot_o[second, last] = gift_ob[...]
    arena[pl.ds(w_rows(second, last), wrow), :] = gift_wb[...]


def store_kernel(n, heads, x, dy, slot_o, arena, y_hbm, dx_hbm, gq_hbm, gk_hbm, gv_hbm, go_hbm, sem_a, sem_b):
    eh, mc = slot_o.shape[2:]
    mh = mc // 2
    wrow = mh * (heads + 2)
    copies = [pltpu.make_async_copy(dy, y_hbm, sem_a.at[0]), pltpu.make_async_copy(x, dx_hbm, sem_a.at[1])]
    for c in range(n):
        for d in range(2):
            dst = go_hbm.at[pl.ds(d * eh, eh), pl.ds(c * mc, mc)]
            copies.append(pltpu.make_async_copy(slot_o.at[d, c], dst, sem_b.at[d, c, 0]))
            row = (d * n + c) * wrow
            start = c * mc + d * mh
            for k, (out, skip, rows) in enumerate(((gq_hbm, 0, heads), (gk_hbm, heads, 1), (gv_hbm, heads + 1, 1))):
                copies.append(pltpu.make_async_copy(
                    arena.at[pl.ds(row + skip * mh, rows * mh)],
                    out.at[pl.ds(start * rows, rows * mh)], sem_b.at[d, c, k + 1],
                ))
    for copy in copies:
        copy.start()
    for copy in copies:
        copy.wait()


def solution(mesh):
    n = mesh.shape["cp"]
    row_spec = P(("dp", "cp"), None)
    rep_spec = P(None, None, None)
    part_spec = P("dp", None, None)

    def device_layer(hidden, grad_out, w_query, w_key, w_value, w_out):
        tok, width = hidden.shape
        heads, hd = w_query.shape[1], w_query.shape[2]
        embed = heads * hd
        kvw = 2 * hd
        half = tok // 2
        cols = heads * half
        mc = width // n
        wrow = mc // 2 * (heads + 2)
        dma = lambda *shape: pltpu.SemaphoreType.DMA(shape)
        ring = dma(2, n - 1)
        split_ring = dma(2, n - 1, 2)
        arena_rows = max(4 * n * tok, 2 * n * wrow)
        state = pl.pallas_call(
            functools.partial(layer_kernel, n, heads),
            name="attention_layer",
            out_shape=[
                pltpu.VMEM((tok, width), BF16),
                pltpu.VMEM((tok, width), BF16),
                pltpu.VMEM((2, n, embed // 2, mc), F32),
                pltpu.VMEM((arena_rows, hd), F32),
            ],
            in_specs=[HBM] * 6,
            out_specs=[VMEM] * 4,
            scratch_shapes=[
                pltpu.VMEM((width, embed + kvw), BF16),
                pltpu.VMEM((embed, width), BF16),
                pltpu.VMEM((n, tok, kvw), BF16),
                pltpu.VMEM((2, cols, hd), BF16),
                pltpu.VMEM((2, hd, cols), BF16),
                pltpu.VMEM((2, cols, hd), BF16),
                pltpu.VMEM((2, hd, cols), BF16),
                pltpu.VMEM((tok, embed), BF16),
                pltpu.VMEM((embed, tok), BF16),
                pltpu.VMEM((2, hd, cols), F32),
                pltpu.VMEM((2, 1, cols), F32),
                pltpu.VMEM((2, 1, cols), F32),
                pltpu.VMEM((2, 1, cols), F32),
                pltpu.VMEM((tok, embed + kvw), BF16),
                pltpu.VMEM((2, embed // 2, mc), F32),
                pltpu.VMEM((2, wrow, hd), F32),
                pltpu.VMEM((mc // 2, tok), BF16),
                pltpu.VMEM((embed // 2, mc), F32),
                pltpu.VMEM((embed // 2, mc), F32),
                pltpu.VMEM((tok, hd), F32),
                pltpu.VMEM((wrow, hd), F32),
                pltpu.VMEM((wrow, hd), F32),
                dma(6),
                dma(2, n // 2), dma(2, n // 2),
                split_ring, split_ring, ring, ring, ring, ring, split_ring, split_ring, split_ring, split_ring,
                dma(5), dma(5),
                pltpu.SemaphoreType.REGULAR,
            ],
            compiler_params=pltpu.CompilerParams(
                collective_id=0, has_side_effects=True, vmem_limit_bytes=30 * 2 ** 20
            ),
        )(
            hidden, grad_out, w_query.reshape(width, embed), w_key.reshape(width, hd), w_value.reshape(width, hd),
            w_out.reshape(embed, width),
        )
        output, grad_hidden, gq, gk, gv, go = pl.pallas_call(
            functools.partial(store_kernel, n, heads),
            name="store_results",
            out_shape=[
                jax.ShapeDtypeStruct((tok, width), BF16),
                jax.ShapeDtypeStruct((tok, width), BF16),
                jax.ShapeDtypeStruct((width * heads, hd), F32),
                jax.ShapeDtypeStruct((width, hd), F32),
                jax.ShapeDtypeStruct((width, hd), F32),
                jax.ShapeDtypeStruct((embed, width), F32),
            ],
            in_specs=[VMEM] * 4,
            out_specs=[HBM] * 6,
            scratch_shapes=[dma(2), dma(2, n, 4)],
            compiler_params=pltpu.CompilerParams(vmem_limit_bytes=2 ** 20),
        )(*state)
        return (
            output,
            grad_hidden,
            gq.reshape(width, heads, hd),
            gk.reshape(width, 1, hd),
            gv.reshape(width, 1, hd),
            go.reshape(heads, hd, width),
        )

    return jax.shard_map(
        device_layer,
        mesh=mesh,
        in_specs=(row_spec, row_spec, rep_spec, rep_spec, rep_spec, rep_spec),
        out_specs=(row_spec, row_spec, part_spec, part_spec, part_spec, part_spec),
        check_vma=False,
    )
```
